32 devices in a mesh: image: 8 (over z, x), space: 4 (over y, core).
Axes of the slice: x: 2, y: 2, z: 4, core: 2. Of those that a mesh axis runs over, the one named last changes fastest.
Arguments:
- magnet: float32 [16, 3, 8, 256, 256], P('image', None, None, 'space'), may hold values from -1 to 1, as said below
- anisotropy: float32 [256], P('space'), may hold values from 0.25 to 10
- kernel: float32 [6, 16, 512, 512], P(None, 'space'), as said below
Outputs:
- updated_magnet: float32 [16, 3, 8, 256, 256], P('image', None, None, 'space')
- band_force: float32 [16, 3, 8, 256, 256], P('image', None, None, 'space')
- energy: float32 [16], P('image')
The draws below stay inside these ranges and needn't reach their ends.
Inputs may be any that keep to these rules, and one draw needn't show every extreme that they name: `magnet`: each cell's three components form a unit vector. `kernel`: each component is even under k -> -k modulo the padded length along every frequency index, except that xy is odd along x and y, xz odd along x and z, and yz odd along y and z.
All inputs are finite; a program needn't handle non-finite values.
Results may differ from the reference program's by a relative error of at most 0.0003.
Values sent between devices are 32-bit elements; how exact they have to be, the bound alone decides.
A program may use at most 256 MiB of HBM per device.

```python
import math
import jax
import jax.numpy as jnp
from jax import lax

NX = 256
NY = 256
NZ = 8
IMAGES = 16


def mirror_part(values, dimension, parity):
    mirrored = jnp.roll(jnp.flip(values, dimension), 1, dimension)
    return 0.5 * (values + parity * mirrored)


def draw_kernel(key, part):
    array_dims = (6, 2 * NZ, 2 * NX, 2 * NY)
    samples = jax.random.normal(key, array_dims, jnp.float32)
    parities = ((1.0, 1.0, 1.0), (1.0, 1.0, 1.0), (1.0, 1.0, 1.0), (-1.0, -1.0, 1.0), (-1.0, 1.0, -1.0), (1.0, -1.0, -1.0))
    components = []
    for component_index in range(6):
        parity_x, parity_y, parity_z = parities[component_index]
        component = mirror_part(samples[component_index], 0, parity_z)
        component = mirror_part(component, 1, parity_x)
        component = mirror_part(component, 2, parity_y)
        if component_index < 3:
            components.append(0.3 + 2.5 * component)
        else:
            components.append(2.0 * component)
    return jnp.stack(components)


def draw_anisotropy(key, part):
    position = jnp.arange(NX, dtype=jnp.float32) / (NX - 1)
    factor = jax.random.uniform(key, (NX,), jnp.float32, 0.5, 2.0)
    return 0.5 * jnp.power(10.0, position) * factor


def draw_magnet(key, part):
    array_dims = (IMAGES, 3, NZ, NX, NY)
    position = jnp.arange(NX, dtype=jnp.float32) / (NX - 1)
    samples = jax.random.normal(key, array_dims, jnp.float32)
    growth = 0.15 * jnp.power(3.0, position)
    lateral = 0.0
    scaled = samples * growth[None, None, None, :, None]
    scaled = scaled.at[0].set(samples[0])
    wandering = jnp.cumsum(scaled, axis=0)
    image_pos = jnp.arange(IMAGES, dtype=jnp.float32) / (IMAGES - 1)
    polar_offset = 2.0 * jnp.cos(math.pi * image_pos)
    offsets = jnp.stack([jnp.zeros_like(polar_offset), jnp.full_like(polar_offset, lateral), polar_offset], axis=1)
    direction = wandering + offsets[:, :, None, None, None]
    return direction / jnp.sqrt(jnp.sum(direction * direction, axis=1, keepdims=True))


def setup_inputs(seed: int = 0) -> dict:
    key_list = jax.random.split(jax.random.key(seed), 4)
    return {
        "magnet": draw_magnet(jax.random.fold_in(key_list[3], 71), 0),
        "anisotropy": draw_anisotropy(jax.random.fold_in(key_list[3], 71), 0),
        "kernel": draw_kernel(jax.random.fold_in(key_list[3], 71), 0),
    }


exchange_strength = 0.25
chiral_strength = 0.3
spring_strength = 10.0
step_limit = 1.0
rotation_limit = 0.5
epsilon = 1e-06

def lift_axes(values):
    return values[:, None, None, None, None]

def total_cells(values):
    return lax.optimization_barrier(jnp.sum(values, axis=tuple(range(1, values.ndim))))

def project(vector, magnet):
    return vector - lax.optimization_barrier(jnp.sum(vector * magnet, axis=1, keepdims=True)) * magnet

def angle_squared(first, second):
    normal_part = jnp.cross(first, second, axis=1)
    sine_value = jnp.sqrt(lax.optimization_barrier(jnp.sum(normal_part * normal_part, axis=1)))
    cosine = lax.optimization_barrier(jnp.sum(first * second, axis=1))
    return jnp.arctan2(sine_value, cosine) ** 2

def tangent_weights(energy_total, energy_next, energy_prior):
    rise_next = energy_next - energy_total
    rise_prior = energy_total - energy_prior
    upward = (rise_next > 0) & (rise_prior > 0)
    downward = (rise_next < 0) & (rise_prior < 0)
    larger = jnp.maximum(jnp.abs(rise_next), jnp.abs(rise_prior))
    smaller = jnp.minimum(jnp.abs(rise_next), jnp.abs(rise_prior))
    toward_next = energy_next > energy_prior
    weight_next = jnp.where(upward, 1.0, jnp.where(downward, 0.0, jnp.where(toward_next, larger, smaller)))
    weight_prior = jnp.where(upward, 0.0, jnp.where(downward, 1.0, jnp.where(toward_next, smaller, larger)))
    return (weight_next, weight_prior)

def local_fields(magnet, anisotropy):
    padded = jnp.pad(magnet, ((0, 0), (0, 0), (1, 1), (1, 1), (1, 1)))
    z_plus = padded[:, :, 2:, 1:-1, 1:-1]
    z_minus = padded[:, :, :-2, 1:-1, 1:-1]
    x_plus = padded[:, :, 1:-1, 2:, 1:-1]
    x_minus = padded[:, :, 1:-1, :-2, 1:-1]
    y_plus = padded[:, :, 1:-1, 1:-1, 2:]
    y_minus = padded[:, :, 1:-1, 1:-1, :-2]
    layer_pos = lax.broadcasted_iota(jnp.int32, (NZ, NX, NY), 0)
    row_pos = lax.broadcasted_iota(jnp.int32, (NZ, NX, NY), 1)
    column_pos = lax.broadcasted_iota(jnp.int32, (NZ, NX, NY), 2)
    boundary = (layer_pos == 0).astype(jnp.float32) + (layer_pos == NZ - 1).astype(jnp.float32)
    boundary = boundary + (row_pos == 0).astype(jnp.float32) + (row_pos == NX - 1).astype(jnp.float32)
    boundary = boundary + (column_pos == 0).astype(jnp.float32) + (column_pos == NY - 1).astype(jnp.float32)
    present = 6.0 - boundary
    neighbours = x_plus + x_minus + y_plus + y_minus + z_plus + z_minus
    exchange_part = exchange_strength * (neighbours - present * magnet)
    chiral_x = chiral_strength * (x_plus[:, 2] - x_minus[:, 2])
    chiral_y = chiral_strength * (y_plus[:, 2] - y_minus[:, 2])
    chiral_z = -chiral_strength * (x_plus[:, 0] - x_minus[:, 0] + (y_plus[:, 1] - y_minus[:, 1]))
    easy_axis = 2.0 * anisotropy[:, None] * magnet[:, 2]
    return exchange_part + jnp.stack([chiral_x, chiral_y, chiral_z + easy_axis], axis=1)

def demag_one(magnet_one, kernel):
    padded = jnp.pad(magnet_one, ((0, 0), (0, NZ), (0, NX), (0, NY)))
    spectrum = jnp.fft.fftn(padded, axes=(1, 2, 3))
    spec_x = spectrum[0]
    spec_y = spectrum[1]
    spec_z = spectrum[2]
    field_x = kernel[0] * spec_x + kernel[3] * spec_y + kernel[4] * spec_z
    field_y = kernel[3] * spec_x + kernel[1] * spec_y + kernel[5] * spec_z
    field_z = kernel[4] * spec_x + kernel[5] * spec_y + kernel[2] * spec_z
    inverse = jnp.fft.ifftn(jnp.stack([field_x, field_y, field_z]), axes=(1, 2, 3))
    return -jnp.real(inverse)[:, :NZ, :NX, :NY]

def reference(magnet, anisotropy, kernel):
    cell_count = NZ * NX * NY

    def one_image(magnet_one):
        return demag_one(magnet_one, kernel)
    demag = lax.map(one_image, magnet)
    fields = local_fields(magnet, anisotropy) + demag
    energy_total = -0.5 * total_cells(magnet * fields)
    next_image = jnp.concatenate([magnet[1:], magnet[-1:]], axis=0)
    prior_image = jnp.concatenate([magnet[:1], magnet[:-1]], axis=0)
    energy_next = jnp.concatenate([energy_total[1:], energy_total[-1:]])
    energy_prior = jnp.concatenate([energy_total[:1], energy_total[:-1]])
    true_force = project(fields, magnet)
    tangent_next = project(next_image - magnet, magnet)
    tangent_prior = project(magnet - prior_image, magnet)
    distance_next = jnp.sqrt(total_cells(angle_squared(magnet, next_image)) / cell_count)
    distance_prior = jnp.sqrt(total_cells(angle_squared(magnet, prior_image)) / cell_count)
    weight_next, weight_prior = tangent_weights(energy_total, energy_next, energy_prior)
    tangent = lift_axes(weight_next) * tangent_next + lift_axes(weight_prior) * tangent_prior
    length_mean = total_cells(tangent * tangent) / cell_count
    unit_tangent = tangent / lift_axes(jnp.sqrt(length_mean + epsilon))
    parallel = total_cells(true_force * unit_tangent) / cell_count
    spring = spring_strength * (distance_next - distance_prior)
    image_index = jnp.arange(IMAGES)
    interior = (image_index > 0) & (image_index < IMAGES - 1)
    band_force = jnp.where(lift_axes(interior), true_force + lift_axes(spring - parallel) * unit_tangent, 0.0)
    largest = lax.optimization_barrier(jnp.max(jnp.sqrt(lax.optimization_barrier(jnp.sum(band_force * band_force, axis=1))), axis=(1, 2, 3)))
    move_scale = jnp.minimum(step_limit, rotation_limit / (largest + epsilon))
    stepped = magnet + lift_axes(move_scale) * band_force
    updated = stepped / jnp.sqrt(lax.optimization_barrier(jnp.sum(stepped * stepped, axis=1, keepdims=True)))
    return (updated, band_force, energy_total / cell_count)
```

```python
import functools
import math

import jax
import jax.numpy as jnp
import numpy as np
from jax import lax
from jax.experimental import pallas as pl
from jax.experimental.pallas import tpu as pltpu
from jax.sharding import PartitionSpec as P

exchange_strength = 0.25
chiral_strength = 0.3
spring_strength = 10.0
step_limit = 1.0
rotation_limit = 0.5
epsilon = 1e-06


def extended(cells, sides, width):
    for axis, dim in sides:
        count = lax.axis_size(axis)
        ends = count - 1
        head = lax.slice_in_dim(cells, 0, width, axis=dim)
        tail = lax.slice_in_dim(cells, cells.shape[dim] - width, cells.shape[dim], axis=dim)
        cells = jnp.concatenate(
            [
                lax.ppermute(tail, axis, [(i, (i + 1) % count) for i in range(ends)]),
                cells,
                lax.ppermute(head, axis, [((i + 1) % count, i) for i in range(ends)]),
            ],
            axis=dim,
        )
    return cells


def lift_axes(values):
    return values[:, None, None, None, None]


def total_cells(values):
    return jnp.sum(values, axis=tuple(range(1, values.ndim)))


def project(vector, magnet):
    return vector - jnp.sum(vector * magnet, axis=1, keepdims=True) * magnet


def angle_squared(first, second):
    normal_part = jnp.cross(first, second, axis=1)
    sine_value = jnp.sqrt(jnp.sum(normal_part * normal_part, axis=1))
    cosine = jnp.sum(first * second, axis=1)
    return jnp.arctan2(sine_value, cosine) ** 2


def tangent_weights(energy_total, energy_next, energy_prior):
    rise_next = energy_next - energy_total
    rise_prior = energy_total - energy_prior
    upward = (rise_next > 0) & (rise_prior > 0)
    downward = (rise_next < 0) & (rise_prior < 0)
    larger = jnp.maximum(jnp.abs(rise_next), jnp.abs(rise_prior))
    smaller = jnp.minimum(jnp.abs(rise_next), jnp.abs(rise_prior))
    toward_next = energy_next > energy_prior
    weight_next = jnp.where(
        upward, 1.0, jnp.where(downward, 0.0, jnp.where(toward_next, larger, smaller))
    )
    weight_prior = jnp.where(
        upward, 0.0, jnp.where(downward, 1.0, jnp.where(toward_next, smaller, larger))
    )
    return (weight_next, weight_prior)


def split_limbs(values):
    upper = values.astype(jnp.bfloat16)
    return upper, (values - upper.astype(jnp.float32)).astype(jnp.bfloat16)


def table_limbs(table):
    upper = table.astype(np.float32).astype(jnp.bfloat16)
    lower = (table - upper.astype(np.float64)).astype(np.float32).astype(jnp.bfloat16)
    return np.stack([upper, lower])


def parity_table(count):
    position = np.arange(count)[:, None]
    slot = np.arange(count)[None, :]
    turn = np.pi / count
    even_part = np.cos(turn * (position * slot % (2 * count)))
    odd_part = np.sin(turn * (position * slot % (2 * count)))
    odd_part[:, 0] = np.cos(turn * (position[:, 0] * count % (2 * count)))
    return np.concatenate([even_part, odd_part], axis=1)


def parity_weights(count):
    weights = np.full((2 * count,), 2.0)
    weights[0] = 1.0
    weights[count] = 1.0
    return weights


def times(value, factor):
    re, im = value
    wr, wi = factor
    if wi == 0.0:
        return (re, im) if wr == 1.0 else (wr * re, wr * im)
    if wr == 0.0:
        return (-im, re) if wi == 1.0 else (-wi * im, wi * re)
    return (wr * re - wi * im, wr * im + wi * re)


def unit_root(index, length, sign):
    quarter = {0: (1.0, 0.0), 1: (0.0, 1.0), 2: (-1.0, 0.0), 3: (0.0, -1.0)}
    if 4 * index % length == 0:
        wr, wi = quarter[4 * index // length % 4]
        return (wr, sign * wi)
    phase = 2.0 * math.pi * index / length
    return (math.cos(phase), sign * math.sin(phase))


def add_pair(first, second):
    return (first[0] + second[0], first[1] + second[1])


def sub_pair(first, second):
    return (first[0] - second[0], first[1] - second[1])


def fourier(values, sign):
    length = len(values)
    if length == 1:
        return values
    evens = fourier(values[0::2], sign)
    odds = fourier(values[1::2], sign)
    half = length // 2
    turned = [times(odds[k], unit_root(k, length, sign)) for k in range(half)]
    return [add_pair(evens[k], turned[k]) for k in range(half)] + [
        sub_pair(evens[k], turned[k]) for k in range(half)
    ]


def layers_to_planes(in_ref, out_ref):
    layer_count = in_ref.shape[2]
    row_step = 8

    def chunk(i, carry):
        rows = pl.ds(pl.multiple_of(i * row_step, row_step), row_step)
        layers = [(in_ref[0, 0, z, rows, :], in_ref[1, 0, z, rows, :]) for z in range(layer_count)]
        turned = [times(layers[z], unit_root(z, 2 * layer_count, -1.0)) for z in range(layer_count)]
        evens = fourier(layers, -1.0)
        odds = fourier(turned, -1.0)
        for k in range(layer_count):
            for part in range(2):
                out_ref[2 * k, 0, part, rows, :] = evens[k][part]
                out_ref[2 * k + 1, 0, part, rows, :] = odds[k][part]
        return carry

    lax.fori_loop(0, in_ref.shape[3] // row_step, chunk, 0)


def planes_to_layers(scale, in_ref, out_ref):
    layer_count = out_ref.shape[2]
    row_step = 8

    def chunk(i, carry):
        rows = pl.ds(pl.multiple_of(i * row_step, row_step), row_step)
        planes = [
            (in_ref[k, 0, 0, rows, :], in_ref[k, 0, 1, rows, :]) for k in range(2 * layer_count)
        ]
        evens = fourier(planes[0::2], 1.0)
        odds = fourier(planes[1::2], 1.0)
        for z in range(layer_count):
            total = add_pair(evens[z], times(odds[z], unit_root(z, 2 * layer_count, 1.0)))
            out_ref[0, 0, z, rows, :] = scale * total[0]
            out_ref[1, 0, z, rows, :] = scale * total[1]
        return carry

    lax.fori_loop(0, out_ref.shape[3] // row_step, chunk, 0)


def dot32(left, right):
    return jnp.dot(left, right, preferred_element_type=jnp.float32)


def plane_kernel(
    in_ref, kernel_ref, fy_ref, fx_ref, gx_ref, gy_ref, out_ref, spec_ref
):
    groups, slab = in_ref.shape[0], in_ref.shape[4]
    rows_full = groups * slab
    columns_full = in_ref.shape[5]

    fy = jnp.concatenate([fy_ref[0], fy_ref[0], fy_ref[1]], axis=0)
    fx = jnp.concatenate([fx_ref[0], fx_ref[0], fx_ref[1]], axis=1)
    gx = jnp.concatenate([gx_ref[0], gx_ref[0], gx_ref[1]], axis=1)
    gy = jnp.concatenate([gy_ref[0], gy_ref[0], gy_ref[1]], axis=0)

    def forward(f, carry):
        c, part = f // 2, f % 2
        cells = jnp.concatenate([in_ref[g, 0, c, part] for g in range(groups)], axis=0)
        upper, lower = split_limbs(cells)
        lines = dot32(jnp.concatenate([upper, lower, upper], axis=1), fy)
        upper, lower = split_limbs(lines)
        spec_ref[f] = dot32(fx, jnp.concatenate([upper, lower, upper], axis=0))
        return carry

    lax.fori_loop(0, 6, forward, 0)

    lane = 128
    sub = 8
    row_pos = lax.broadcasted_iota(jnp.int32, (sub, lane), 0)
    lane_pos = lax.broadcasted_iota(jnp.int32, (sub, lane), 1)

    def tensor(i, carry):
        row_start = pl.multiple_of(i * sub, sub)
        top = (row_pos + row_start) == 0
        for start in range(0, columns_full, lane):

            def pick(component, odd_x, odd_y):
                def at(rows):
                    inner = kernel_ref[component, 0, rows, start : start + lane]
                    if odd_y and start == 0:
                        edge = kernel_ref[component, 0, rows, columns_full : columns_full + lane]
                        inner = jnp.where(lane_pos == 0, edge, inner)
                    return inner

                values = at(pl.ds(row_start, sub))
                if odd_x:
                    values = jnp.where(top, at(pl.ds(rows_full, sub)), values)
                return values

            spec = {}
            for px in range(2):
                for py in range(2):
                    for f in range(6):
                        spec[px, py, f] = spec_ref[
                            f,
                            pl.ds(row_start + px * rows_full, sub),
                            py * columns_full + start : py * columns_full + start + lane,
                        ]
            k_xy = pick(3, 0, 0)
            for px in range(2):
                for py in range(2):
                    sx = 1.0 if px else -1.0
                    sy = 1.0 if py else -1.0
                    k_xx, k_yy, k_zz = [pick(n, px, py) for n in range(3)]
                    k_xz = sx * pick(4, 0, py)
                    k_yz = sy * pick(5, px, 0)
                    xy_both = -(sx * sy) * k_xy
                    for part in range(2):
                        turn = 1.0 if part else -1.0
                        other = 1 - part
                        field_x = (
                            k_xx * spec[px, py, part]
                            + xy_both * spec[1 - px, 1 - py, 2 + part]
                            + turn * (k_xz * spec[1 - px, py, 4 + other])
                        )
                        field_y = (
                            xy_both * spec[1 - px, 1 - py, part]
                            + k_yy * spec[px, py, 2 + part]
                            + turn * (k_yz * spec[px, 1 - py, 4 + other])
                        )
                        field_z = k_zz * spec[px, py, 4 + part] + turn * (
                            k_xz * spec[1 - px, py, other] + k_yz * spec[px, 1 - py, 2 + other]
                        )
                        for c, field in enumerate((field_x, field_y, field_z)):
                            spec_ref[
                                2 * c + part,
                                pl.ds(row_start + px * rows_full, sub),
                                py * columns_full + start : py * columns_full + start + lane,
                            ] = field
        return carry

    lax.fori_loop(0, rows_full // sub, tensor, 0)

    def backward(f, carry):
        c, part = f // 2, f % 2
        upper, lower = split_limbs(spec_ref[f])
        lines = dot32(gx, jnp.concatenate([upper, lower, upper], axis=0))
        upper, lower = split_limbs(lines)
        cells = dot32(jnp.concatenate([upper, lower, upper], axis=1), gy)
        for g in range(groups):
            out_ref[g, 0, c, part] = cells[g * slab : (g + 1) * slab]
        return carry

    lax.fori_loop(0, 6, backward, 0)


def demag_pair(magnet, kernel):
    layer_count, row_count, column_count = magnet.shape[2:]
    groups = lax.axis_size("space")
    local_planes = 2 * layer_count // groups
    full_rows = row_count * groups
    plane_dims = (2 * layer_count, 3, 2, row_count, column_count)
    layer_spec = pl.BlockSpec((2, 1, layer_count, row_count, column_count), lambda c: (0, c, 0, 0, 0))
    plane_spec = pl.BlockSpec((2 * layer_count, 1, 2, row_count, column_count), lambda c: (0, c, 0, 0, 0))
    planes = pl.pallas_call(
        layers_to_planes,
        grid=(3,),
        in_specs=[layer_spec],
        out_specs=plane_spec,
        out_shape=jax.ShapeDtypeStruct(plane_dims, jnp.float32),
        name="layers_to_planes",
    )(magnet)
    planes = lax.all_to_all(planes, "space", split_axis=0, concat_axis=0, tiled=True)
    planes = planes.reshape((groups, local_planes) + plane_dims[1:])
    table_y = parity_table(column_count)
    table_x = parity_table(full_rows)
    tables = [
        table_limbs(table_y),
        table_limbs(table_x.T),
        table_limbs(table_x * parity_weights(full_rows)[None, :]),
        table_limbs((table_y * parity_weights(column_count)[None, :]).T),
    ]
    slab_spec = pl.BlockSpec(
        (groups, 1, 3, 2, row_count, column_count), lambda q: (0, q, 0, 0, 0, 0)
    )
    kernel_spec = pl.BlockSpec(
        (6, 1, full_rows + 8, column_count + 128), lambda q: (0, q, 0, 0)
    )
    whole_spec = [pl.BlockSpec(t.shape, lambda q: (0, 0, 0)) for t in tables]
    planes = pl.pallas_call(
        plane_kernel,
        grid=(local_planes,),
        in_specs=[slab_spec, kernel_spec] + whole_spec,
        out_specs=slab_spec,
        out_shape=jax.ShapeDtypeStruct(planes.shape, jnp.float32),
        scratch_shapes=[
            pltpu.VMEM((6, 2 * full_rows, 2 * column_count), jnp.float32),
        ],
        compiler_params=pltpu.CompilerParams(vmem_limit_bytes=60 * 1024 * 1024),
        name="plane_kernel",
    )(planes, kernel, *[jnp.asarray(t) for t in tables])
    planes = planes.reshape(plane_dims)
    planes = lax.all_to_all(planes, "space", split_axis=0, concat_axis=0, tiled=True)
    padded_cells = 8 * layer_count * full_rows * column_count
    return pl.pallas_call(
        functools.partial(planes_to_layers, -1.0 / padded_cells),
        grid=(3,),
        in_specs=[plane_spec],
        out_specs=layer_spec,
        out_shape=jax.ShapeDtypeStruct(magnet.shape, jnp.float32),
        name="planes_to_layers",
    )(planes)


def demag_field(magnet, kernel):
    pairs = [
        demag_pair(magnet[start : start + 2], kernel) for start in range(0, magnet.shape[0], 2)
    ]
    return pairs[0] if len(pairs) == 1 else jnp.concatenate(pairs, axis=0)


def local_fields(magnet, anisotropy, kernel):
    layer_count = magnet.shape[2]
    row_count = magnet.shape[3]
    column_count = magnet.shape[4]
    rimmed = extended(magnet, (("space", 3),), 1)
    x_plus = rimmed[:, :, :, 2:]
    x_minus = rimmed[:, :, :, :-2]
    padded = jnp.pad(magnet, ((0, 0), (0, 0), (1, 1), (0, 0), (1, 1)))
    z_plus = padded[:, :, 2:, :, 1:-1]
    z_minus = padded[:, :, :-2, :, 1:-1]
    y_plus = padded[:, :, 1:-1, :, 2:]
    y_minus = padded[:, :, 1:-1, :, :-2]
    first_row = lax.axis_index("space") * row_count
    full_rows = row_count * lax.axis_size("space")
    layer_pos = lax.broadcasted_iota(jnp.int32, (layer_count, row_count, column_count), 0)
    row_pos = lax.broadcasted_iota(jnp.int32, (layer_count, row_count, column_count), 1) + first_row
    column_pos = lax.broadcasted_iota(jnp.int32, (layer_count, row_count, column_count), 2)
    boundary = (layer_pos == 0).astype(jnp.float32) + (layer_pos == layer_count - 1).astype(
        jnp.float32
    )
    boundary = (
        boundary
        + (row_pos == 0).astype(jnp.float32)
        + (row_pos == full_rows - 1).astype(jnp.float32)
    )
    boundary = (
        boundary
        + (column_pos == 0).astype(jnp.float32)
        + (column_pos == column_count - 1).astype(jnp.float32)
    )
    present = 6.0 - boundary
    neighbours = x_plus + x_minus + y_plus + y_minus + z_plus + z_minus
    exchange_part = exchange_strength * (neighbours - present * magnet)
    chiral_x = chiral_strength * (x_plus[:, 2] - x_minus[:, 2])
    chiral_y = chiral_strength * (y_plus[:, 2] - y_minus[:, 2])
    chiral_z = -chiral_strength * (x_plus[:, 0] - x_minus[:, 0] + (y_plus[:, 1] - y_minus[:, 1]))
    easy_axis = 2.0 * anisotropy[:, None] * magnet[:, 2]
    local_part = exchange_part + jnp.stack([chiral_x, chiral_y, chiral_z + easy_axis], axis=1)
    return local_part + demag_field(magnet, kernel)


def body(magnet, anisotropy, kernel):
    image_count = magnet.shape[0]
    cell_count = magnet.shape[2] * magnet.shape[3] * lax.axis_size("space") * magnet.shape[4]
    fields = local_fields(magnet, anisotropy, kernel)
    framed = extended(magnet, (("image", 0),), 1)
    prior_image = framed[:-2]
    next_image = framed[2:]
    true_force = project(fields, magnet)
    tangent_next = project(next_image - magnet, magnet)
    tangent_prior = project(magnet - prior_image, magnet)
    energy_part = -0.5 * total_cells(magnet * fields)
    next_part = total_cells(angle_squared(magnet, next_image))
    prior_part = total_cells(angle_squared(magnet, prior_image))
    energy_total, next_squares, prior_squares = lax.psum(
        (energy_part, next_part, prior_part), "space"
    )
    framed_energy = extended(energy_total, (("image", 0),), 1)
    weight_next, weight_prior = tangent_weights(energy_total, framed_energy[2:], framed_energy[:-2])
    tangent = lift_axes(weight_next) * tangent_next + lift_axes(weight_prior) * tangent_prior
    length_squares, drive_total = lax.psum(
        (total_cells(tangent * tangent), total_cells(true_force * tangent)), "space"
    )
    tangent_scale = jnp.sqrt(length_squares / cell_count + epsilon)
    unit_tangent = tangent / lift_axes(tangent_scale)
    parallel = drive_total / (cell_count * tangent_scale)
    distance_next = jnp.sqrt(next_squares / cell_count)
    distance_prior = jnp.sqrt(prior_squares / cell_count)
    spring = spring_strength * (distance_next - distance_prior)
    image_index = lax.axis_index("image") * image_count + jnp.arange(image_count)
    band_size = image_count * lax.axis_size("image")
    interior = (image_index > 0) & (image_index < band_size - 1)
    band_force = jnp.where(
        lift_axes(interior), true_force + lift_axes(spring - parallel) * unit_tangent, 0.0
    )
    local_largest = jnp.max(jnp.sqrt(jnp.sum(band_force * band_force, axis=1)), axis=(1, 2, 3))
    largest = lax.pmax(local_largest, "space")
    move_scale = jnp.minimum(step_limit, rotation_limit / (largest + epsilon))
    stepped = magnet + lift_axes(move_scale) * band_force
    updated = stepped / jnp.sqrt(jnp.sum(stepped * stepped, axis=1, keepdims=True))
    return (updated, band_force, energy_total / cell_count)


def solution(mesh):
    in_specs = (P("image", None, None, "space", None), P("space"), P(None, "space", None, None))
    out_specs = (
        P("image", None, None, "space", None),
        P("image", None, None, "space", None),
        P("image"),
    )
    return jax.shard_map(body, mesh=mesh, in_specs=in_specs, out_specs=out_specs, check_vma=False)
```

```python
import functools
import math

import jax
import jax.numpy as jnp
import numpy as np
from jax import lax
from jax.experimental import pallas as pl
from jax.experimental.pallas import tpu as pltpu
from jax.sharding import PartitionSpec as P

exchange_strength = 0.25
chiral_strength = 0.3
spring_strength = 10.0
step_limit = 1.0
rotation_limit = 0.5
epsilon = 1e-06


def extended(cells, sides, width):
    for axis, dim in sides:
        count = lax.axis_size(axis)
        ends = count - 1
        head = lax.slice_in_dim(cells, 0, width, axis=dim)
        tail = lax.slice_in_dim(cells, cells.shape[dim] - width, cells.shape[dim], axis=dim)
        cells = jnp.concatenate(
            [
                lax.ppermute(tail, axis, [(i, (i + 1) % count) for i in range(ends)]),
                cells,
                lax.ppermute(head, axis, [((i + 1) % count, i) for i in range(ends)]),
            ],
            axis=dim,
        )
    return cells


def lift_axes(values):
    return values[:, None, None, None, None]


def total_cells(values):
    return jnp.sum(values, axis=tuple(range(1, values.ndim)))


def project(vector, magnet):
    return vector - jnp.sum(vector * magnet, axis=1, keepdims=True) * magnet


def angle_squared(first, second):
    normal_part = jnp.cross(first, second, axis=1)
    sine_value = jnp.sqrt(jnp.sum(normal_part * normal_part, axis=1))
    cosine = jnp.sum(first * second, axis=1)
    return jnp.arctan2(sine_value, cosine) ** 2


def tangent_weights(energy_total, energy_next, energy_prior):
    rise_next = energy_next - energy_total
    rise_prior = energy_total - energy_prior
    upward = (rise_next > 0) & (rise_prior > 0)
    downward = (rise_next < 0) & (rise_prior < 0)
    larger = jnp.maximum(jnp.abs(rise_next), jnp.abs(rise_prior))
    smaller = jnp.minimum(jnp.abs(rise_next), jnp.abs(rise_prior))
    toward_next = energy_next > energy_prior
    weight_next = jnp.where(
        upward, 1.0, jnp.where(downward, 0.0, jnp.where(toward_next, larger, smaller))
    )
    weight_prior = jnp.where(
        upward, 0.0, jnp.where(downward, 1.0, jnp.where(toward_next, smaller, larger))
    )
    return (weight_next, weight_prior)


def split_limbs(values):
    upper = values.astype(jnp.bfloat16)
    return upper, (values - upper.astype(jnp.float32)).astype(jnp.bfloat16)


def table_limbs(table):
    upper = table.astype(np.float32).astype(jnp.bfloat16)
    lower = (table - upper.astype(np.float64)).astype(np.float32).astype(jnp.bfloat16)
    return np.stack([upper, lower])


def parity_table(count):
    position = np.arange(count)[:, None]
    slot = np.arange(count)[None, :]
    turn = np.pi / count
    even_part = np.cos(turn * (position * slot % (2 * count)))
    odd_part = np.sin(turn * (position * slot % (2 * count)))
    odd_part[:, 0] = np.cos(turn * (position[:, 0] * count % (2 * count)))
    return np.concatenate([even_part, odd_part], axis=1)


def parity_weights(count):
    weights = np.full((2 * count,), 2.0)
    weights[0] = 1.0
    weights[count] = 1.0
    return weights


def times(value, factor):
    re, im = value
    wr, wi = factor
    if wi == 0.0:
        return (re, im) if wr == 1.0 else (wr * re, wr * im)
    if wr == 0.0:
        return (-im, re) if wi == 1.0 else (-wi * im, wi * re)
    return (wr * re - wi * im, wr * im + wi * re)


def unit_root(index, length, sign):
    quarter = {0: (1.0, 0.0), 1: (0.0, 1.0), 2: (-1.0, 0.0), 3: (0.0, -1.0)}
    if 4 * index % length == 0:
        wr, wi = quarter[4 * index // length % 4]
        return (wr, sign * wi)
    phase = 2.0 * math.pi * index / length
    return (math.cos(phase), sign * math.sin(phase))


def add_pair(first, second):
    return (first[0] + second[0], first[1] + second[1])


def sub_pair(first, second):
    return (first[0] - second[0], first[1] - second[1])


def fourier(values, sign):
    length = len(values)
    if length == 1:
        return values
    evens = fourier(values[0::2], sign)
    odds = fourier(values[1::2], sign)
    half = length // 2
    turned = [times(odds[k], unit_root(k, length, sign)) for k in range(half)]
    return [add_pair(evens[k], turned[k]) for k in range(half)] + [
        sub_pair(evens[k], turned[k]) for k in range(half)
    ]


def layers_to_planes(in_ref, out_ref):
    layer_count = in_ref.shape[2]
    row_step = 8

    def chunk(i, carry):
        rows = pl.ds(pl.multiple_of(i * row_step, row_step), row_step)
        layers = [(in_ref[0, 0, z, rows, :], in_ref[1, 0, z, rows, :]) for z in range(layer_count)]
        turned = [times(layers[z], unit_root(z, 2 * layer_count, -1.0)) for z in range(layer_count)]
        evens = fourier(layers, -1.0)
        odds = fourier(turned, -1.0)
        for k in range(layer_count):
            for part in range(2):
                out_ref[2 * k, 0, part, rows, :] = evens[k][part]
                out_ref[2 * k + 1, 0, part, rows, :] = odds[k][part]
        return carry

    lax.fori_loop(0, in_ref.shape[3] // row_step, chunk, 0)


def planes_to_layers(scale, in_ref, out_ref):
    layer_count = out_ref.shape[2]
    row_step = 8

    def chunk(i, carry):
        rows = pl.ds(pl.multiple_of(i * row_step, row_step), row_step)
        planes = [
            (in_ref[k, 0, 0, rows, :], in_ref[k, 0, 1, rows, :]) for k in range(2 * layer_count)
        ]
        evens = fourier(planes[0::2], 1.0)
        odds = fourier(planes[1::2], 1.0)
        for z in range(layer_count):
            total = add_pair(evens[z], times(odds[z], unit_root(z, 2 * layer_count, 1.0)))
            out_ref[0, 0, z, rows, :] = scale * total[0]
            out_ref[1, 0, z, rows, :] = scale * total[1]
        return carry

    lax.fori_loop(0, out_ref.shape[3] // row_step, chunk, 0)


def dot32(left, right):
    return jnp.dot(left, right, preferred_element_type=jnp.float32)


def plane_kernel(
    planes_ref,
    kernel_ref,
    fy_ref,
    fx_ref,
    gx_ref,
    gy_ref,
    out_ref,
    spec_ref,
    held_ref,
    tensor_ref,
    result_ref,
    send_sem,
    recv_sem,
    own_sem,
    tensor_sem,
    out_sem,
):
    groups, local_planes = planes_ref.shape[0], planes_ref.shape[1]
    slab, columns_full = planes_ref.shape[4], planes_ref.shape[5]
    rows_full = groups * slab
    me = lax.axis_index("space")
    peers = [lax.rem(me + d, groups) for d in range(groups)]
    sources = [lax.rem(me + groups - d, groups) for d in range(groups)]

    def tensor_copy(q):
        return pltpu.make_async_copy(
            kernel_ref.at[:, q, pl.ds(0, rows_full + 8), pl.ds(0, columns_full + 128)],
            tensor_ref.at[q],
            tensor_sem.at[q],
        )

    def own_copy(q):
        return pltpu.make_async_copy(planes_ref.at[me, q], held_ref.at[q, me], own_sem.at[q])

    def out_copy(q):
        return pltpu.make_async_copy(result_ref.at[q], out_ref.at[:, q], out_sem.at[q])

    def remote_copy(q, d):
        return pltpu.make_async_remote_copy(
            src_ref=planes_ref.at[peers[d], q],
            dst_ref=held_ref.at[q, me],
            send_sem=send_sem.at[q, d],
            recv_sem=recv_sem.at[q, d],
            device_id={"space": peers[d]},
            device_id_type=pl.DeviceIdType.MESH,
        )

    def arrival(q, d):
        return pltpu.make_async_remote_copy(
            src_ref=planes_ref.at[peers[d], q],
            dst_ref=held_ref.at[q, sources[d]],
            send_sem=send_sem.at[q, d],
            recv_sem=recv_sem.at[q, d],
            device_id={"space": peers[d]},
            device_id_type=pl.DeviceIdType.MESH,
        )

    barrier = pltpu.get_barrier_semaphore()
    for d in range(1, groups):
        pl.semaphore_signal(
            barrier, inc=1, device_id={"space": peers[d]}, device_id_type=pl.DeviceIdType.MESH
        )
    for q in range(local_planes):
        tensor_copy(q).start()
        own_copy(q).start()
    pl.semaphore_wait(barrier, groups - 1)
    for q in range(local_planes):
        for d in range(1, groups):
            remote_copy(q, d).start()

    def plane(q, carry):
        tensor_copy(q).wait()
        own_copy(q).wait()
        for d in range(1, groups):
            arrival(q, d).wait_recv()
        plane_compute(
            held_ref.at[q], tensor_ref.at[q], fy_ref, fx_ref, gx_ref, gy_ref, result_ref.at[q], spec_ref
        )
        out_copy(q).start()
        return carry

    lax.fori_loop(0, local_planes, plane, 0)
    for q in range(local_planes):
        out_copy(q).wait()
        for d in range(1, groups):
            remote_copy(q, d).wait_send()


def plane_compute(in_ref, kernel_ref, fy_ref, fx_ref, gx_ref, gy_ref, out_ref, spec_ref):
    groups, slab, columns_full = in_ref.shape[0], in_ref.shape[3], in_ref.shape[4]
    rows_full = groups * slab
    fy = jnp.concatenate([fy_ref[0], fy_ref[0], fy_ref[1]], axis=0)
    fx = jnp.concatenate([fx_ref[0], fx_ref[0], fx_ref[1]], axis=1)
    gx = jnp.concatenate([gx_ref[0], gx_ref[0], gx_ref[1]], axis=1)
    gy = jnp.concatenate([gy_ref[0], gy_ref[0], gy_ref[1]], axis=0)

    def forward(f, carry):
        c, part = f // 2, f % 2
        cells = jnp.concatenate([in_ref[g, c, part] for g in range(groups)], axis=0)
        upper, lower = split_limbs(cells)
        lines = dot32(jnp.concatenate([upper, lower, upper], axis=1), fy)
        upper, lower = split_limbs(lines)
        spec_ref[f] = dot32(fx, jnp.concatenate([upper, lower, upper], axis=0))
        return carry

    lax.fori_loop(0, 6, forward, 0)

    lane = 128
    sub = 8
    row_pos = lax.broadcasted_iota(jnp.int32, (sub, lane), 0)
    lane_pos = lax.broadcasted_iota(jnp.int32, (sub, lane), 1)

    def tensor(i, carry):
        row_start = pl.multiple_of(i * sub, sub)
        top = (row_pos + row_start) == 0
        for start in range(0, columns_full, lane):

            def pick(component, odd_x, odd_y):
                def at(rows):
                    inner = kernel_ref[component, rows, start : start + lane]
                    if odd_y and start == 0:
                        edge = kernel_ref[component, rows, columns_full : columns_full + lane]
                        inner = jnp.where(lane_pos == 0, edge, inner)
                    return inner

                values = at(pl.ds(row_start, sub))
                if odd_x:
                    values = jnp.where(top, at(pl.ds(rows_full, sub)), values)
                return values

            spec = {}
            for px in range(2):
                for py in range(2):
                    for f in range(6):
                        spec[px, py, f] = spec_ref[
                            f,
                            pl.ds(row_start + px * rows_full, sub),
                            py * columns_full + start : py * columns_full + start + lane,
                        ]
            k_xy = pick(3, 0, 0)
            for px in range(2):
                for py in range(2):
                    sx = 1.0 if px else -1.0
                    sy = 1.0 if py else -1.0
                    k_xx, k_yy, k_zz = [pick(n, px, py) for n in range(3)]
                    k_xz = sx * pick(4, 0, py)
                    k_yz = sy * pick(5, px, 0)
                    xy_both = -(sx * sy) * k_xy
                    for part in range(2):
                        turn = 1.0 if part else -1.0
                        other = 1 - part
                        field_x = (
                            k_xx * spec[px, py, part]
                            + xy_both * spec[1 - px, 1 - py, 2 + part]
                            + turn * (k_xz * spec[1 - px, py, 4 + other])
                        )
                        field_y = (
                            xy_both * spec[1 - px, 1 - py, part]
                            + k_yy * spec[px, py, 2 + part]
                            + turn * (k_yz * spec[px, 1 - py, 4 + other])
                        )
                        field_z = k_zz * spec[px, py, 4 + part] + turn * (
                            k_xz * spec[1 - px, py, other] + k_yz * spec[px, 1 - py, 2 + other]
                        )
                        for c, field in enumerate((field_x, field_y, field_z)):
                            spec_ref[
                                2 * c + part,
                                pl.ds(row_start + px * rows_full, sub),
                                py * columns_full + start : py * columns_full + start + lane,
                            ] = field
        return carry

    lax.fori_loop(0, rows_full // sub, tensor, 0)

    def backward(f, carry):
        c, part = f // 2, f % 2
        upper, lower = split_limbs(spec_ref[f])
        lines = dot32(gx, jnp.concatenate([upper, lower, upper], axis=0))
        upper, lower = split_limbs(lines)
        cells = dot32(jnp.concatenate([upper, lower, upper], axis=1), gy)
        for g in range(groups):
            out_ref[g, c, part] = cells[g * slab : (g + 1) * slab]
        return carry

    lax.fori_loop(0, 6, backward, 0)


def demag_pair(magnet, kernel, images, pair_index):
    layer_count, row_count, column_count = magnet.shape[2:]
    groups = lax.axis_size("space")
    local_planes = 2 * layer_count // groups
    full_rows = row_count * groups
    plane_dims = (2 * layer_count, 3, 2, row_count, column_count)
    layer_spec = pl.BlockSpec((2, 1, layer_count, row_count, column_count), lambda c: (0, c, 0, 0, 0))
    plane_spec = pl.BlockSpec((2 * layer_count, 1, 2, row_count, column_count), lambda c: (0, c, 0, 0, 0))
    planes = pl.pallas_call(
        layers_to_planes,
        grid=(3,),
        in_specs=[layer_spec],
        out_specs=plane_spec,
        out_shape=jax.ShapeDtypeStruct(plane_dims, jnp.float32),
        name="layers_to_planes",
    )(magnet)
    planes = planes.reshape((groups, local_planes) + plane_dims[1:])
    table_y = parity_table(column_count)
    table_x = parity_table(full_rows)
    tables = [
        table_limbs(table_y),
        table_limbs(table_x.T),
        table_limbs(table_x * parity_weights(full_rows)[None, :]),
        table_limbs((table_y * parity_weights(column_count)[None, :]).T),
    ]
    slab_dims = (local_planes, groups, 3, 2, row_count, column_count)
    tensor_dims = (local_planes, 6, full_rows + 8, column_count + 128)
    anywhere = pl.BlockSpec(memory_space=pl.ANY)
    inside = pl.BlockSpec(memory_space=pltpu.VMEM)
    dots = 6 * local_planes * 4 * full_rows * column_count * 3 * (full_rows + column_count // 2)
    planes = pl.pallas_call(
        plane_kernel,
        in_specs=[anywhere, anywhere] + [inside] * len(tables),
        out_specs=anywhere,
        out_shape=jax.ShapeDtypeStruct(planes.shape, jnp.float32),
        scratch_shapes=[
            pltpu.VMEM((6, 2 * full_rows, 2 * column_count), jnp.float32),
            pltpu.VMEM(slab_dims, jnp.float32),
            pltpu.VMEM(tensor_dims, jnp.float32),
            pltpu.VMEM(slab_dims, jnp.float32),
            pltpu.SemaphoreType.DMA((local_planes, groups)),
            pltpu.SemaphoreType.DMA((local_planes, groups)),
            pltpu.SemaphoreType.DMA((local_planes,)),
            pltpu.SemaphoreType.DMA((local_planes,)),
            pltpu.SemaphoreType.DMA((local_planes,)),
        ],
        compiler_params=pltpu.CompilerParams(
            vmem_limit_bytes=56 * 1024 * 1024, collective_id=pair_index, has_side_effects=True
        ),
        cost_estimate=pl.CostEstimate(
            flops=4 * dots, bytes_accessed=4 * planes.size * 4, transcendentals=0
        ),
        name="plane_kernel",
    )(planes, kernel, *[jnp.asarray(t) for t in tables])
    planes = planes.reshape(plane_dims)
    planes, *images = lax.optimization_barrier((planes, *images))
    planes = lax.all_to_all(planes, "space", split_axis=0, concat_axis=0, tiled=True)
    padded_cells = 8 * layer_count * full_rows * column_count
    field = pl.pallas_call(
        functools.partial(planes_to_layers, -1.0 / padded_cells),
        grid=(3,),
        in_specs=[plane_spec],
        out_specs=layer_spec,
        out_shape=jax.ShapeDtypeStruct(magnet.shape, jnp.float32),
        name="planes_to_layers",
    )(planes)
    return field, images


def demag_field(magnet, kernel, images):
    fields = []
    for index, start in enumerate(range(0, magnet.shape[0], 2)):
        field, images = demag_pair(magnet[start : start + 2], kernel, images, index)
        fields.append(field)
    return (fields[0] if len(fields) == 1 else jnp.concatenate(fields, axis=0)), images


def local_fields(magnet, anisotropy):
    layer_count = magnet.shape[2]
    row_count = magnet.shape[3]
    column_count = magnet.shape[4]
    rimmed = extended(magnet, (("space", 3),), 1)
    x_plus = rimmed[:, :, :, 2:]
    x_minus = rimmed[:, :, :, :-2]
    padded = jnp.pad(magnet, ((0, 0), (0, 0), (1, 1), (0, 0), (1, 1)))
    z_plus = padded[:, :, 2:, :, 1:-1]
    z_minus = padded[:, :, :-2, :, 1:-1]
    y_plus = padded[:, :, 1:-1, :, 2:]
    y_minus = padded[:, :, 1:-1, :, :-2]
    first_row = lax.axis_index("space") * row_count
    full_rows = row_count * lax.axis_size("space")
    layer_pos = lax.broadcasted_iota(jnp.int32, (layer_count, row_count, column_count), 0)
    row_pos = lax.broadcasted_iota(jnp.int32, (layer_count, row_count, column_count), 1) + first_row
    column_pos = lax.broadcasted_iota(jnp.int32, (layer_count, row_count, column_count), 2)
    boundary = (layer_pos == 0).astype(jnp.float32) + (layer_pos == layer_count - 1).astype(
        jnp.float32
    )
    boundary = (
        boundary
        + (row_pos == 0).astype(jnp.float32)
        + (row_pos == full_rows - 1).astype(jnp.float32)
    )
    boundary = (
        boundary
        + (column_pos == 0).astype(jnp.float32)
        + (column_pos == column_count - 1).astype(jnp.float32)
    )
    present = 6.0 - boundary
    neighbours = x_plus + x_minus + y_plus + y_minus + z_plus + z_minus
    exchange_part = exchange_strength * (neighbours - present * magnet)
    chiral_x = chiral_strength * (x_plus[:, 2] - x_minus[:, 2])
    chiral_y = chiral_strength * (y_plus[:, 2] - y_minus[:, 2])
    chiral_z = -chiral_strength * (x_plus[:, 0] - x_minus[:, 0] + (y_plus[:, 1] - y_minus[:, 1]))
    easy_axis = 2.0 * anisotropy[:, None] * magnet[:, 2]
    local_part = exchange_part + jnp.stack([chiral_x, chiral_y, chiral_z + easy_axis], axis=1)
    return local_part


def body(magnet, anisotropy, kernel):
    image_count = magnet.shape[0]
    cell_count = magnet.shape[2] * magnet.shape[3] * lax.axis_size("space") * magnet.shape[4]
    framed = extended(magnet, (("image", 0),), 1)
    demag, (framed,) = demag_field(magnet, kernel, [framed])
    fields = local_fields(magnet, anisotropy) + demag
    prior_image = framed[:-2]
    next_image = framed[2:]
    true_force = project(fields, magnet)
    tangent_next = project(next_image - magnet, magnet)
    tangent_prior = project(magnet - prior_image, magnet)
    sums = jnp.stack(
        [
            -0.5 * total_cells(magnet * fields),
            total_cells(angle_squared(magnet, next_image)),
            total_cells(tangent_next * tangent_next),
            total_cells(tangent_next * tangent_prior),
            total_cells(tangent_prior * tangent_prior),
            total_cells(true_force * tangent_next),
            total_cells(true_force * tangent_prior),
        ],
        axis=1,
    )
    band_size = image_count * lax.axis_size("image")
    gathered = lax.all_gather(sums, ("image", "space"))
    gathered = gathered.reshape(
        (lax.axis_size("image"), lax.axis_size("space")) + sums.shape
    )
    band = jnp.sum(gathered, axis=1).reshape(band_size, sums.shape[1])
    energy_band, distance_band = band[:, 0], jnp.sqrt(band[:, 1] / cell_count)
    weight_next, weight_prior = tangent_weights(
        energy_band, jnp.roll(energy_band, -1), jnp.roll(energy_band, 1)
    )
    length_squares = (
        weight_next * weight_next * band[:, 2]
        + 2.0 * weight_next * weight_prior * band[:, 3]
        + weight_prior * weight_prior * band[:, 4]
    )
    drive_total = weight_next * band[:, 5] + weight_prior * band[:, 6]
    tangent_scale = jnp.sqrt(jnp.maximum(length_squares, 0.0) / cell_count + epsilon)
    parallel = drive_total / (cell_count * tangent_scale)
    spring = spring_strength * (distance_band - jnp.roll(distance_band, 1))
    image_index = jnp.arange(band_size)
    interior = ((image_index > 0) & (image_index < band_size - 1)).astype(jnp.float32)
    pull = (spring - parallel) / tangent_scale
    first_image = lax.axis_index("image") * image_count
    mine = lax.dynamic_slice_in_dim(
        jnp.stack([energy_band, pull * weight_next, pull * weight_prior, interior], axis=1),
        first_image,
        image_count,
        axis=0,
    )
    energy_total = mine[:, 0]
    band_force = jnp.where(
        lift_axes(mine[:, 3]) > 0.0,
        true_force + lift_axes(mine[:, 1]) * tangent_next + lift_axes(mine[:, 2]) * tangent_prior,
        0.0,
    )
    local_largest = jnp.max(jnp.sqrt(jnp.sum(band_force * band_force, axis=1)), axis=(1, 2, 3))
    largest = lax.pmax(local_largest, "space")
    move_scale = jnp.minimum(step_limit, rotation_limit / (largest + epsilon))
    stepped = magnet + lift_axes(move_scale) * band_force
    updated = stepped / jnp.sqrt(jnp.sum(stepped * stepped, axis=1, keepdims=True))
    return (updated, band_force, energy_total / cell_count)


def solution(mesh):
    in_specs = (P("image", None, None, "space", None), P("space"), P(None, "space", None, None))
    out_specs = (
        P("image", None, None, "space", None),
        P("image", None, None, "space", None),
        P("image"),
    )
    return jax.shard_map(body, mesh=mesh, in_specs=in_specs, out_specs=out_specs, check_vma=False)
```

```python
import functools
import math

import jax
import jax.numpy as jnp
import numpy as np
from jax import lax
from jax.experimental import pallas as pl
from jax.experimental.pallas import tpu as pltpu
from jax.sharding import PartitionSpec as P

exchange_strength = 0.25
chiral_strength = 0.3
spring_strength = 10.0
step_limit = 1.0
rotation_limit = 0.5
epsilon = 1e-06


def extended(cells, sides, width):
    for axis, dim in sides:
        count = lax.axis_size(axis)
        ends = count - 1
        head = lax.slice_in_dim(cells, 0, width, axis=dim)
        tail = lax.slice_in_dim(cells, cells.shape[dim] - width, cells.shape[dim], axis=dim)
        cells = jnp.concatenate(
            [
                lax.ppermute(tail, axis, [(i, (i + 1) % count) for i in range(ends)]),
                cells,
                lax.ppermute(head, axis, [((i + 1) % count, i) for i in range(ends)]),
            ],
            axis=dim,
        )
    return cells


def lift_axes(values):
    return values[:, None, None, None, None]


def total_cells(values):
    return jnp.sum(values, axis=tuple(range(1, values.ndim)))


def project(vector, magnet):
    return vector - jnp.sum(vector * magnet, axis=1, keepdims=True) * magnet


def angle_squared(first, second):
    normal_part = jnp.cross(first, second, axis=1)
    sine_value = jnp.sqrt(jnp.sum(normal_part * normal_part, axis=1))
    cosine = jnp.sum(first * second, axis=1)
    return jnp.arctan2(sine_value, cosine) ** 2


def tangent_weights(energy_total, energy_next, energy_prior):
    rise_next = energy_next - energy_total
    rise_prior = energy_total - energy_prior
    upward = (rise_next > 0) & (rise_prior > 0)
    downward = (rise_next < 0) & (rise_prior < 0)
    larger = jnp.maximum(jnp.abs(rise_next), jnp.abs(rise_prior))
    smaller = jnp.minimum(jnp.abs(rise_next), jnp.abs(rise_prior))
    toward_next = energy_next > energy_prior
    weight_next = jnp.where(
        upward, 1.0, jnp.where(downward, 0.0, jnp.where(toward_next, larger, smaller))
    )
    weight_prior = jnp.where(
        upward, 0.0, jnp.where(downward, 1.0, jnp.where(toward_next, smaller, larger))
    )
    return (weight_next, weight_prior)


def split_limbs(values):
    upper = values.astype(jnp.bfloat16)
    return upper, (values - upper.astype(jnp.float32)).astype(jnp.bfloat16)


def table_limbs(table):
    upper = table.astype(np.float32).astype(jnp.bfloat16)
    lower = (table - upper.astype(np.float64)).astype(np.float32).astype(jnp.bfloat16)
    return np.stack([upper, lower])


def parity_table(count):
    position = np.arange(count)[:, None]
    slot = np.arange(count)[None, :]
    turn = np.pi / count
    even_part = np.cos(turn * (position * slot % (2 * count)))
    odd_part = np.sin(turn * (position * slot % (2 * count)))
    odd_part[:, 0] = np.cos(turn * (position[:, 0] * count % (2 * count)))
    return np.concatenate([even_part, odd_part], axis=1)


def parity_weights(count):
    weights = np.full((2 * count,), 2.0)
    weights[0] = 1.0
    weights[count] = 1.0
    return weights


def times(value, factor):
    re, im = value
    wr, wi = factor
    if wi == 0.0:
        return (re, im) if wr == 1.0 else (wr * re, wr * im)
    if wr == 0.0:
        return (-im, re) if wi == 1.0 else (-wi * im, wi * re)
    return (wr * re - wi * im, wr * im + wi * re)


def unit_root(index, length, sign):
    quarter = {0: (1.0, 0.0), 1: (0.0, 1.0), 2: (-1.0, 0.0), 3: (0.0, -1.0)}
    if 4 * index % length == 0:
        wr, wi = quarter[4 * index // length % 4]
        return (wr, sign * wi)
    phase = 2.0 * math.pi * index / length
    return (math.cos(phase), sign * math.sin(phase))


def add_pair(first, second):
    return (first[0] + second[0], first[1] + second[1])


def sub_pair(first, second):
    return (first[0] - second[0], first[1] - second[1])


def fourier(values, sign):
    length = len(values)
    if length == 1:
        return values
    evens = fourier(values[0::2], sign)
    odds = fourier(values[1::2], sign)
    half = length // 2
    turned = [times(odds[k], unit_root(k, length, sign)) for k in range(half)]
    return [add_pair(evens[k], turned[k]) for k in range(half)] + [
        sub_pair(evens[k], turned[k]) for k in range(half)
    ]


def layers_to_planes(in_ref, out_ref):
    layer_count = in_ref.shape[2]
    row_step = 8

    def chunk(i, carry):
        rows = pl.ds(pl.multiple_of(i * row_step, row_step), row_step)
        layers = [(in_ref[0, 0, z, rows, :], in_ref[1, 0, z, rows, :]) for z in range(layer_count)]
        turned = [times(layers[z], unit_root(z, 2 * layer_count, -1.0)) for z in range(layer_count)]
        evens = fourier(layers, -1.0)
        odds = fourier(turned, -1.0)
        for k in range(layer_count):
            for part in range(2):
                out_ref[2 * k, 0, part, rows, :] = evens[k][part]
                out_ref[2 * k + 1, 0, part, rows, :] = odds[k][part]
        return carry

    lax.fori_loop(0, in_ref.shape[3] // row_step, chunk, 0)


def planes_to_layers(scale, in_ref, out_ref):
    layer_count = out_ref.shape[2]
    row_step = 8

    def chunk(i, carry):
        rows = pl.ds(pl.multiple_of(i * row_step, row_step), row_step)
        planes = [
            (in_ref[k, 0, 0, rows, :], in_ref[k, 0, 1, rows, :]) for k in range(2 * layer_count)
        ]
        evens = fourier(planes[0::2], 1.0)
        odds = fourier(planes[1::2], 1.0)
        for z in range(layer_count):
            total = add_pair(evens[z], times(odds[z], unit_root(z, 2 * layer_count, 1.0)))
            out_ref[0, 0, z, rows, :] = scale * total[0]
            out_ref[1, 0, z, rows, :] = scale * total[1]
        return carry

    lax.fori_loop(0, out_ref.shape[3] // row_step, chunk, 0)


def dot32(left, right):
    return jnp.dot(left, right, preferred_element_type=jnp.float32)


def plane_kernel(
    planes_ref,
    kernel_ref,
    fy_ref,
    fx_ref,
    gx_ref,
    gy_ref,
    out_ref,
    spec_ref,
    held_ref,
    tensor_ref,
    result_ref,
    send_sem,
    recv_sem,
    own_sem,
    tensor_sem,
    out_sem,
):
    groups, local_planes = planes_ref.shape[0], planes_ref.shape[1]
    slab, columns_full = planes_ref.shape[4], planes_ref.shape[5]
    rows_full = groups * slab
    me = lax.axis_index("space")
    peers = [lax.rem(me + d, groups) for d in range(groups)]
    sources = [lax.rem(me + groups - d, groups) for d in range(groups)]

    def tensor_copy(q):
        return pltpu.make_async_copy(
            kernel_ref.at[:, q, pl.ds(0, rows_full + 8), pl.ds(0, columns_full + 128)],
            tensor_ref.at[q],
            tensor_sem.at[q],
        )

    def own_copy(q):
        return pltpu.make_async_copy(planes_ref.at[me, q], held_ref.at[q, me], own_sem.at[q])

    def out_copy(q):
        return pltpu.make_async_copy(result_ref.at[q], out_ref.at[:, q], out_sem.at[q])

    def remote_copy(q, d):
        return pltpu.make_async_remote_copy(
            src_ref=planes_ref.at[peers[d], q],
            dst_ref=held_ref.at[q, me],
            send_sem=send_sem.at[q, d],
            recv_sem=recv_sem.at[q, d],
            device_id={"space": peers[d]},
            device_id_type=pl.DeviceIdType.MESH,
        )

    def arrival(q, d):
        return pltpu.make_async_remote_copy(
            src_ref=planes_ref.at[peers[d], q],
            dst_ref=held_ref.at[q, sources[d]],
            send_sem=send_sem.at[q, d],
            recv_sem=recv_sem.at[q, d],
            device_id={"space": peers[d]},
            device_id_type=pl.DeviceIdType.MESH,
        )

    barrier = pltpu.get_barrier_semaphore()
    for d in range(1, groups):
        pl.semaphore_signal(
            barrier, inc=1, device_id={"space": peers[d]}, device_id_type=pl.DeviceIdType.MESH
        )
    for q in range(local_planes):
        tensor_copy(q).start()
        own_copy(q).start()
    pl.semaphore_wait(barrier, groups - 1)
    for q in range(local_planes):
        for d in range(1, groups):
            remote_copy(q, d).start()

    def plane(q, carry):
        tensor_copy(q).wait()
        own_copy(q).wait()
        for d in range(1, groups):
            arrival(q, d).wait_recv()
        plane_compute(
            held_ref.at[q], tensor_ref.at[q], fy_ref, fx_ref, gx_ref, gy_ref, result_ref.at[q], spec_ref
        )
        out_copy(q).start()
        return carry

    lax.fori_loop(0, local_planes, plane, 0)
    for q in range(local_planes):
        out_copy(q).wait()
        for d in range(1, groups):
            remote_copy(q, d).wait_send()


def plane_compute(in_ref, kernel_ref, fy_ref, fx_ref, gx_ref, gy_ref, out_ref, spec_ref):
    groups, slab, columns_full = in_ref.shape[0], in_ref.shape[3], in_ref.shape[4]
    rows_full = groups * slab
    fy = jnp.concatenate([fy_ref[0], fy_ref[0], fy_ref[1]], axis=0)
    fx = jnp.concatenate([fx_ref[0], fx_ref[0], fx_ref[1]], axis=1)
    gx = jnp.concatenate([gx_ref[0], gx_ref[0], gx_ref[1]], axis=1)
    gy = jnp.concatenate([gy_ref[0], gy_ref[0], gy_ref[1]], axis=0)

    def forward(f, carry):
        c, part = f // 2, f % 2
        cells = jnp.concatenate([in_ref[g, c, part] for g in range(groups)], axis=0)
        upper, lower = split_limbs(cells)
        lines = dot32(jnp.concatenate([upper, lower, upper], axis=1), fy)
        upper, lower = split_limbs(lines)
        spec_ref[f] = dot32(fx, jnp.concatenate([upper, lower, upper], axis=0))
        return carry

    lax.fori_loop(0, 6, forward, 0)

    lane = 128
    sub = 8
    row_pos = lax.broadcasted_iota(jnp.int32, (sub, lane), 0)
    lane_pos = lax.broadcasted_iota(jnp.int32, (sub, lane), 1)

    def tensor(i, carry):
        row_start = pl.multiple_of(i * sub, sub)
        top = (row_pos + row_start) == 0
        for start in range(0, columns_full, lane):

            def pick(component, odd_x, odd_y):
                def at(rows):
                    inner = kernel_ref[component, rows, start : start + lane]
                    if odd_y and start == 0:
                        edge = kernel_ref[component, rows, columns_full : columns_full + lane]
                        inner = jnp.where(lane_pos == 0, edge, inner)
                    return inner

                values = at(pl.ds(row_start, sub))
                if odd_x:
                    values = jnp.where(top, at(pl.ds(rows_full, sub)), values)
                return values

            spec = {}
            for px in range(2):
                for py in range(2):
                    for f in range(6):
                        spec[px, py, f] = spec_ref[
                            f,
                            pl.ds(row_start + px * rows_full, sub),
                            py * columns_full + start : py * columns_full + start + lane,
                        ]
            k_xy = pick(3, 0, 0)
            for px in range(2):
                for py in range(2):
                    sx = 1.0 if px else -1.0
                    sy = 1.0 if py else -1.0
                    k_xx, k_yy, k_zz = [pick(n, px, py) for n in range(3)]
                    k_xz = sx * pick(4, 0, py)
                    k_yz = sy * pick(5, px, 0)
                    xy_both = -(sx * sy) * k_xy
                    for part in range(2):
                        turn = 1.0 if part else -1.0
                        other = 1 - part
                        field_x = (
                            k_xx * spec[px, py, part]
                            + xy_both * spec[1 - px, 1 - py, 2 + part]
                            + turn * (k_xz * spec[1 - px, py, 4 + other])
                        )
                        field_y = (
                            xy_both * spec[1 - px, 1 - py, part]
                            + k_yy * spec[px, py, 2 + part]
                            + turn * (k_yz * spec[px, 1 - py, 4 + other])
                        )
                        field_z = k_zz * spec[px, py, 4 + part] + turn * (
                            k_xz * spec[1 - px, py, other] + k_yz * spec[px, 1 - py, 2 + other]
                        )
                        for c, field in enumerate((field_x, field_y, field_z)):
                            spec_ref[
                                2 * c + part,
                                pl.ds(row_start + px * rows_full, sub),
                                py * columns_full + start : py * columns_full + start + lane,
                            ] = field
        return carry

    lax.fori_loop(0, rows_full // sub, tensor, 0)

    def backward(f, carry):
        c, part = f // 2, f % 2
        upper, lower = split_limbs(spec_ref[f])
        lines = dot32(gx, jnp.concatenate([upper, lower, upper], axis=0))
        upper, lower = split_limbs(lines)
        cells = dot32(jnp.concatenate([upper, lower, upper], axis=1), gy)
        for g in range(groups):
            out_ref[g, c, part] = cells[g * slab : (g + 1) * slab]
        return carry

    lax.fori_loop(0, 6, backward, 0)


def swap_kernel(shifts, combine, tile_ref, out_ref, held_ref, send_sem, recv_sem):
    groups, images = lax.axis_size("space"), lax.axis_size("image")
    me, image = lax.axis_index("space"), lax.axis_index("image")
    routes = [
        (n, shift, d)
        for n, shift in enumerate(shifts)
        for d in range(groups)
        if shift != 0 or d != 0
    ]

    def target(shift, d):
        return {"image": lax.rem(image - shift + images, images), "space": lax.rem(me + d, groups)}

    barrier = pltpu.get_barrier_semaphore()
    for n, shift, d in routes:
        pl.semaphore_signal(
            barrier, inc=1, device_id=target(shift, d), device_id_type=pl.DeviceIdType.MESH
        )
    pl.semaphore_wait(barrier, len(routes))

    def copy_of(n, shift, d, slot):
        return pltpu.make_async_remote_copy(
            src_ref=tile_ref,
            dst_ref=held_ref.at[n, slot],
            send_sem=send_sem.at[n, d],
            recv_sem=recv_sem.at[n, d],
            device_id=target(shift, d),
            device_id_type=pl.DeviceIdType.MESH,
        )

    for n, shift, d in routes:
        copy_of(n, shift, d, me).start()
    held_ref[shifts.index(0), me] = tile_ref[...]
    for n, shift, d in routes:
        copy_of(n, shift, d, lax.rem(me + groups - d, groups)).wait_recv()
    for n in range(len(shifts)):
        total = held_ref[n, 0]
        for g in range(1, groups):
            total = combine(total, held_ref[n, g])
        out_ref[n] = total
    for n, shift, d in routes:
        copy_of(n, shift, d, me).wait_send()


def swapped(values, shifts, combine, collective_id):
    rows, columns = values.shape
    tile = jnp.pad(values, ((0, -rows % 8), (0, -columns % 128)))
    groups = lax.axis_size("space")
    inside = pl.BlockSpec(memory_space=pltpu.VMEM)
    result = pl.pallas_call(
        functools.partial(swap_kernel, shifts, combine),
        in_specs=[inside],
        out_specs=inside,
        out_shape=jax.ShapeDtypeStruct((len(shifts),) + tile.shape, jnp.float32),
        scratch_shapes=[
            pltpu.VMEM((len(shifts), groups) + tile.shape, jnp.float32),
            pltpu.SemaphoreType.DMA((len(shifts), groups)),
            pltpu.SemaphoreType.DMA((len(shifts), groups)),
        ],
        compiler_params=pltpu.CompilerParams(
            collective_id=collective_id, has_side_effects=True
        ),
        name="swap_kernel",
    )(tile)
    return result[:, :rows, :columns]


def demag_pair(magnet, kernel, images, early_work, pair_index):
    layer_count, row_count, column_count = magnet.shape[2:]
    groups = lax.axis_size("space")
    local_planes = 2 * layer_count // groups
    full_rows = row_count * groups
    plane_dims = (2 * layer_count, 3, 2, row_count, column_count)
    layer_spec = pl.BlockSpec((2, 1, layer_count, row_count, column_count), lambda c: (0, c, 0, 0, 0))
    plane_spec = pl.BlockSpec((2 * layer_count, 1, 2, row_count, column_count), lambda c: (0, c, 0, 0, 0))
    planes = pl.pallas_call(
        layers_to_planes,
        grid=(3,),
        in_specs=[layer_spec],
        out_specs=plane_spec,
        out_shape=jax.ShapeDtypeStruct(plane_dims, jnp.float32),
        name="layers_to_planes",
    )(magnet)
    planes = planes.reshape((groups, local_planes) + plane_dims[1:])
    table_y = parity_table(column_count)
    table_x = parity_table(full_rows)
    tables = [
        table_limbs(table_y),
        table_limbs(table_x.T),
        table_limbs(table_x * parity_weights(full_rows)[None, :]),
        table_limbs((table_y * parity_weights(column_count)[None, :]).T),
    ]
    slab_dims = (local_planes, groups, 3, 2, row_count, column_count)
    tensor_dims = (local_planes, 6, full_rows + 8, column_count + 128)
    anywhere = pl.BlockSpec(memory_space=pl.ANY)
    inside = pl.BlockSpec(memory_space=pltpu.VMEM)
    dots = 6 * local_planes * 4 * full_rows * column_count * 3 * (full_rows + column_count // 2)
    planes = pl.pallas_call(
        plane_kernel,
        in_specs=[anywhere, anywhere] + [inside] * len(tables),
        out_specs=anywhere,
        out_shape=jax.ShapeDtypeStruct(planes.shape, jnp.float32),
        scratch_shapes=[
            pltpu.VMEM((6, 2 * full_rows, 2 * column_count), jnp.float32),
            pltpu.VMEM(slab_dims, jnp.float32),
            pltpu.VMEM(tensor_dims, jnp.float32),
            pltpu.VMEM(slab_dims, jnp.float32),
            pltpu.SemaphoreType.DMA((local_planes, groups)),
            pltpu.SemaphoreType.DMA((local_planes, groups)),
            pltpu.SemaphoreType.DMA((local_planes,)),
            pltpu.SemaphoreType.DMA((local_planes,)),
            pltpu.SemaphoreType.DMA((local_planes,)),
        ],
        compiler_params=pltpu.CompilerParams(
            vmem_limit_bytes=56 * 1024 * 1024, collective_id=pair_index, has_side_effects=True
        ),
        cost_estimate=pl.CostEstimate(
            flops=4 * dots, bytes_accessed=4 * planes.size * 4, transcendentals=0
        ),
        name="plane_kernel",
    )(planes, kernel, *[jnp.asarray(t) for t in tables])
    planes = planes.reshape(plane_dims)
    planes, *images = lax.optimization_barrier((planes, *images))
    planes = lax.all_to_all(planes, "space", split_axis=0, concat_axis=0, tiled=True)
    planes, early = lax.optimization_barrier((planes, early_work(images)))
    padded_cells = 8 * layer_count * full_rows * column_count
    field = pl.pallas_call(
        functools.partial(planes_to_layers, -1.0 / padded_cells),
        grid=(3,),
        in_specs=[plane_spec],
        out_specs=layer_spec,
        out_shape=jax.ShapeDtypeStruct(magnet.shape, jnp.float32),
        name="planes_to_layers",
    )(planes)
    return field, images, early


def demag_field(magnet, kernel, images, early_work):
    fields = []
    for index, start in enumerate(range(0, magnet.shape[0], 2)):
        field, images, early = demag_pair(
            magnet[start : start + 2], kernel, images, early_work, index
        )
        fields.append(field)
    return (fields[0] if len(fields) == 1 else jnp.concatenate(fields, axis=0)), images, early


def local_fields(magnet, anisotropy):
    layer_count = magnet.shape[2]
    row_count = magnet.shape[3]
    column_count = magnet.shape[4]
    rimmed = extended(magnet, (("space", 3),), 1)
    x_plus = rimmed[:, :, :, 2:]
    x_minus = rimmed[:, :, :, :-2]
    padded = jnp.pad(magnet, ((0, 0), (0, 0), (1, 1), (0, 0), (1, 1)))
    z_plus = padded[:, :, 2:, :, 1:-1]
    z_minus = padded[:, :, :-2, :, 1:-1]
    y_plus = padded[:, :, 1:-1, :, 2:]
    y_minus = padded[:, :, 1:-1, :, :-2]
    first_row = lax.axis_index("space") * row_count
    full_rows = row_count * lax.axis_size("space")
    layer_pos = lax.broadcasted_iota(jnp.int32, (layer_count, row_count, column_count), 0)
    row_pos = lax.broadcasted_iota(jnp.int32, (layer_count, row_count, column_count), 1) + first_row
    column_pos = lax.broadcasted_iota(jnp.int32, (layer_count, row_count, column_count), 2)
    boundary = (layer_pos == 0).astype(jnp.float32) + (layer_pos == layer_count - 1).astype(
        jnp.float32
    )
    boundary = (
        boundary
        + (row_pos == 0).astype(jnp.float32)
        + (row_pos == full_rows - 1).astype(jnp.float32)
    )
    boundary = (
        boundary
        + (column_pos == 0).astype(jnp.float32)
        + (column_pos == column_count - 1).astype(jnp.float32)
    )
    present = 6.0 - boundary
    neighbours = x_plus + x_minus + y_plus + y_minus + z_plus + z_minus
    exchange_part = exchange_strength * (neighbours - present * magnet)
    chiral_x = chiral_strength * (x_plus[:, 2] - x_minus[:, 2])
    chiral_y = chiral_strength * (y_plus[:, 2] - y_minus[:, 2])
    chiral_z = -chiral_strength * (x_plus[:, 0] - x_minus[:, 0] + (y_plus[:, 1] - y_minus[:, 1]))
    easy_axis = 2.0 * anisotropy[:, None] * magnet[:, 2]
    local_part = exchange_part + jnp.stack([chiral_x, chiral_y, chiral_z + easy_axis], axis=1)
    return local_part


def body(magnet, anisotropy, kernel):
    image_count = magnet.shape[0]
    cell_count = magnet.shape[2] * magnet.shape[3] * lax.axis_size("space") * magnet.shape[4]
    framed = extended(magnet, (("image", 0),), 1)

    def early_work(images):
        prior, following = images[0][:-2], images[0][2:]
        ahead = project(following - magnet, magnet)
        behind = project(magnet - prior, magnet)
        return (
            local_fields(magnet, anisotropy),
            total_cells(angle_squared(magnet, following)),
            total_cells(ahead * ahead),
            total_cells(ahead * behind),
            total_cells(behind * behind),
        )

    demag, (framed,), early = demag_field(magnet, kernel, [framed], early_work)
    fields = early[0] + demag
    prior_image = framed[:-2]
    next_image = framed[2:]
    true_force = project(fields, magnet)
    tangent_next = project(next_image - magnet, magnet)
    tangent_prior = project(magnet - prior_image, magnet)
    sums = jnp.stack(
        [
            -0.5 * total_cells(magnet * fields),
            *early[1:],
            total_cells(true_force * tangent_next),
            total_cells(true_force * tangent_prior),
        ],
        axis=1,
    )
    band_size = image_count * lax.axis_size("image")
    swaps = swapped(sums, (-1, 0, 1), jnp.add, 64)
    band = jnp.concatenate([swaps[0, -1:], swaps[1], swaps[2, :1]], axis=0)
    energy_band, distance_band = band[:, 0], jnp.sqrt(band[:, 1] / cell_count)
    weight_next, weight_prior = tangent_weights(
        energy_band, jnp.roll(energy_band, -1), jnp.roll(energy_band, 1)
    )
    length_squares = (
        weight_next * weight_next * band[:, 2]
        + 2.0 * weight_next * weight_prior * band[:, 3]
        + weight_prior * weight_prior * band[:, 4]
    )
    drive_total = weight_next * band[:, 5] + weight_prior * band[:, 6]
    tangent_scale = jnp.sqrt(jnp.maximum(length_squares, 0.0) / cell_count + epsilon)
    parallel = drive_total / (cell_count * tangent_scale)
    spring = spring_strength * (distance_band - jnp.roll(distance_band, 1))
    first_image = lax.axis_index("image") * image_count
    image_index = first_image - 1 + jnp.arange(image_count + 2)
    interior = ((image_index > 0) & (image_index < band_size - 1)).astype(jnp.float32)
    pull = (spring - parallel) / tangent_scale
    mine = jnp.stack([energy_band, pull * weight_next, pull * weight_prior, interior], axis=1)[1:-1]
    energy_total = mine[:, 0]
    band_force = jnp.where(
        lift_axes(mine[:, 3]) > 0.0,
        true_force + lift_axes(mine[:, 1]) * tangent_next + lift_axes(mine[:, 2]) * tangent_prior,
        0.0,
    )
    local_largest = jnp.max(jnp.sqrt(jnp.sum(band_force * band_force, axis=1)), axis=(1, 2, 3))
    largest = swapped(local_largest[None, :], (0,), jnp.maximum, 65)[0, 0]
    move_scale = jnp.minimum(step_limit, rotation_limit / (largest + epsilon))
    stepped = magnet + lift_axes(move_scale) * band_force
    updated = stepped / jnp.sqrt(jnp.sum(stepped * stepped, axis=1, keepdims=True))
    return (updated, band_force, energy_total / cell_count)


def solution(mesh):
    in_specs = (P("image", None, None, "space", None), P("space"), P(None, "space", None, None))
    out_specs = (
        P("image", None, None, "space", None),
        P("image", None, None, "space", None),
        P("image"),
    )
    return jax.shard_map(body, mesh=mesh, in_specs=in_specs, out_specs=out_specs, check_vma=False)
```

```python
import functools
import math

import jax
import jax.numpy as jnp
import numpy as np
from jax import lax
from jax.experimental import pallas as pl
from jax.experimental.pallas import tpu as pltpu
from jax.sharding import PartitionSpec as P

exchange_strength = 0.25
chiral_strength = 0.3
spring_strength = 10.0
step_limit = 1.0
rotation_limit = 0.5
epsilon = 1e-06


def extended(cells, sides, width):
    for axis, dim in sides:
        count = lax.axis_size(axis)
        ends = count - 1
        head = lax.slice_in_dim(cells, 0, width, axis=dim)
        tail = lax.slice_in_dim(cells, cells.shape[dim] - width, cells.shape[dim], axis=dim)
        cells = jnp.concatenate(
            [
                lax.ppermute(tail, axis, [(i, (i + 1) % count) for i in range(ends)]),
                cells,
                lax.ppermute(head, axis, [((i + 1) % count, i) for i in range(ends)]),
            ],
            axis=dim,
        )
    return cells


def lift_axes(values):
    return values[:, None, None, None, None]


def total_cells(values):
    return jnp.sum(values, axis=tuple(range(1, values.ndim)))


def project(vector, magnet):
    return vector - jnp.sum(vector * magnet, axis=1, keepdims=True) * magnet


def angle_squared(first, second):
    normal_part = jnp.cross(first, second, axis=1)
    sine_value = jnp.sqrt(jnp.sum(normal_part * normal_part, axis=1))
    cosine = jnp.sum(first * second, axis=1)
    return jnp.arctan2(sine_value, cosine) ** 2


def tangent_weights(energy_total, energy_next, energy_prior):
    rise_next = energy_next - energy_total
    rise_prior = energy_total - energy_prior
    upward = (rise_next > 0) & (rise_prior > 0)
    downward = (rise_next < 0) & (rise_prior < 0)
    larger = jnp.maximum(jnp.abs(rise_next), jnp.abs(rise_prior))
    smaller = jnp.minimum(jnp.abs(rise_next), jnp.abs(rise_prior))
    toward_next = energy_next > energy_prior
    weight_next = jnp.where(
        upward, 1.0, jnp.where(downward, 0.0, jnp.where(toward_next, larger, smaller))
    )
    weight_prior = jnp.where(
        upward, 0.0, jnp.where(downward, 1.0, jnp.where(toward_next, smaller, larger))
    )
    return (weight_next, weight_prior)


def split_limbs(values):
    upper = values.astype(jnp.bfloat16)
    return upper, (values - upper.astype(jnp.float32)).astype(jnp.bfloat16)


def table_limbs(table):
    upper = table.astype(np.float32).astype(jnp.bfloat16)
    lower = (table - upper.astype(np.float64)).astype(np.float32).astype(jnp.bfloat16)
    return np.stack([upper, lower])


def parity_table(count):
    position = np.arange(count)[:, None]
    slot = np.arange(count)[None, :]
    turn = np.pi / count
    even_part = np.cos(turn * (position * slot % (2 * count)))
    odd_part = np.sin(turn * (position * slot % (2 * count)))
    odd_part[:, 0] = np.cos(turn * (position[:, 0] * count % (2 * count)))
    return np.concatenate([even_part, odd_part], axis=1)


def parity_weights(count):
    weights = np.full((2 * count,), 2.0)
    weights[0] = 1.0
    weights[count] = 1.0
    return weights


def times(value, factor):
    re, im = value
    wr, wi = factor
    if wi == 0.0:
        return (re, im) if wr == 1.0 else (wr * re, wr * im)
    if wr == 0.0:
        return (-im, re) if wi == 1.0 else (-wi * im, wi * re)
    return (wr * re - wi * im, wr * im + wi * re)


def unit_root(index, length, sign):
    quarter = {0: (1.0, 0.0), 1: (0.0, 1.0), 2: (-1.0, 0.0), 3: (0.0, -1.0)}
    if 4 * index % length == 0:
        wr, wi = quarter[4 * index // length % 4]
        return (wr, sign * wi)
    phase = 2.0 * math.pi * index / length
    return (math.cos(phase), sign * math.sin(phase))


def add_pair(first, second):
    return (first[0] + second[0], first[1] + second[1])


def sub_pair(first, second):
    return (first[0] - second[0], first[1] - second[1])


def fourier(values, sign):
    length = len(values)
    if length == 1:
        return values
    evens = fourier(values[0::2], sign)
    odds = fourier(values[1::2], sign)
    half = length // 2
    turned = [times(odds[k], unit_root(k, length, sign)) for k in range(half)]
    return [add_pair(evens[k], turned[k]) for k in range(half)] + [
        sub_pair(evens[k], turned[k]) for k in range(half)
    ]


def layers_to_planes(in_ref, out_ref):
    layer_count = in_ref.shape[2]
    row_step = 8

    def chunk(i, carry):
        rows = pl.ds(pl.multiple_of(i * row_step, row_step), row_step)
        layers = [(in_ref[0, 0, z, rows, :], in_ref[1, 0, z, rows, :]) for z in range(layer_count)]
        turned = [times(layers[z], unit_root(z, 2 * layer_count, -1.0)) for z in range(layer_count)]
        evens = fourier(layers, -1.0)
        odds = fourier(turned, -1.0)
        for k in range(layer_count):
            for part in range(2):
                out_ref[2 * k, 0, part, rows, :] = evens[k][part]
                out_ref[2 * k + 1, 0, part, rows, :] = odds[k][part]
        return carry

    lax.fori_loop(0, in_ref.shape[3] // row_step, chunk, 0)


def planes_to_layers(scale, in_ref, out_ref):
    layer_count = out_ref.shape[2]
    row_step = 8

    def chunk(i, carry):
        rows = pl.ds(pl.multiple_of(i * row_step, row_step), row_step)
        planes = [
            (in_ref[k, 0, 0, rows, :], in_ref[k, 0, 1, rows, :]) for k in range(2 * layer_count)
        ]
        evens = fourier(planes[0::2], 1.0)
        odds = fourier(planes[1::2], 1.0)
        for z in range(layer_count):
            total = add_pair(evens[z], times(odds[z], unit_root(z, 2 * layer_count, 1.0)))
            out_ref[0, 0, z, rows, :] = scale * total[0]
            out_ref[1, 0, z, rows, :] = scale * total[1]
        return carry

    lax.fori_loop(0, out_ref.shape[3] // row_step, chunk, 0)


def dot32(left, right):
    return jnp.dot(left, right, preferred_element_type=jnp.float32)


def plane_kernel(
    planes_ref,
    kernel_ref,
    fy_ref,
    fx_ref,
    gx_ref,
    gy_ref,
    out_ref,
    spec_ref,
    held_ref,
    tensor_ref,
    result_ref,
    send_sem,
    recv_sem,
    own_sem,
    tensor_sem,
    out_sem,
):
    groups, local_planes = planes_ref.shape[0], planes_ref.shape[1]
    slab, columns_full = planes_ref.shape[4], planes_ref.shape[5]
    rows_full = groups * slab
    me = lax.axis_index("space")
    peers = [lax.rem(me + d, groups) for d in range(groups)]
    sources = [lax.rem(me + groups - d, groups) for d in range(groups)]

    def tensor_copy(q):
        return pltpu.make_async_copy(
            kernel_ref.at[:, q, pl.ds(0, rows_full + 8), pl.ds(0, columns_full + 128)],
            tensor_ref.at[q],
            tensor_sem.at[q],
        )

    def own_copy(q):
        return pltpu.make_async_copy(planes_ref.at[me, q], held_ref.at[q, me], own_sem.at[q])

    def out_copy(q):
        return pltpu.make_async_copy(result_ref.at[q], out_ref.at[:, q], out_sem.at[q])

    def remote_copy(q, d):
        return pltpu.make_async_remote_copy(
            src_ref=planes_ref.at[peers[d], q],
            dst_ref=held_ref.at[q, me],
            send_sem=send_sem.at[q, d],
            recv_sem=recv_sem.at[q, d],
            device_id={"space": peers[d]},
            device_id_type=pl.DeviceIdType.MESH,
        )

    def arrival(q, d):
        return pltpu.make_async_remote_copy(
            src_ref=planes_ref.at[peers[d], q],
            dst_ref=held_ref.at[q, sources[d]],
            send_sem=send_sem.at[q, d],
            recv_sem=recv_sem.at[q, d],
            device_id={"space": peers[d]},
            device_id_type=pl.DeviceIdType.MESH,
        )

    barrier = pltpu.get_barrier_semaphore()
    for d in range(1, groups):
        pl.semaphore_signal(
            barrier, inc=1, device_id={"space": peers[d]}, device_id_type=pl.DeviceIdType.MESH
        )
    for q in range(local_planes):
        tensor_copy(q).start()
        own_copy(q).start()
    pl.semaphore_wait(barrier, groups - 1)
    for q in range(local_planes):
        for d in range(1, groups):
            remote_copy(q, d).start()

    def plane(q, carry):
        tensor_copy(q).wait()
        own_copy(q).wait()
        for d in range(1, groups):
            arrival(q, d).wait_recv()
        plane_compute(
            held_ref.at[q], tensor_ref.at[q], fy_ref, fx_ref, gx_ref, gy_ref, result_ref.at[q], spec_ref
        )
        out_copy(q).start()
        return carry

    lax.fori_loop(0, local_planes, plane, 0)
    for q in range(local_planes):
        out_copy(q).wait()
        for d in range(1, groups):
            remote_copy(q, d).wait_send()


def plane_compute(in_ref, kernel_ref, fy_ref, fx_ref, gx_ref, gy_ref, out_ref, spec_ref):
    groups, slab, columns_full = in_ref.shape[0], in_ref.shape[3], in_ref.shape[4]
    rows_full = groups * slab
    fy = jnp.concatenate([fy_ref[0], fy_ref[0], fy_ref[1]], axis=0)
    fx = jnp.concatenate([fx_ref[0], fx_ref[0], fx_ref[1]], axis=1)
    gx = jnp.concatenate([gx_ref[0], gx_ref[0], gx_ref[1]], axis=1)
    gy = jnp.concatenate([gy_ref[0], gy_ref[0], gy_ref[1]], axis=0)

    def forward(f, carry):
        c, part = f // 2, f % 2
        cells = jnp.concatenate([in_ref[g, c, part] for g in range(groups)], axis=0)
        upper, lower = split_limbs(cells)
        lines = dot32(jnp.concatenate([upper, lower, upper], axis=1), fy)
        upper, lower = split_limbs(lines)
        spec_ref[f] = dot32(fx, jnp.concatenate([upper, lower, upper], axis=0))
        return carry

    lax.fori_loop(0, 6, forward, 0)

    lane = 128
    sub = 8
    row_pos = lax.broadcasted_iota(jnp.int32, (sub, lane), 0)
    lane_pos = lax.broadcasted_iota(jnp.int32, (sub, lane), 1)

    def tensor(i, carry):
        row_start = pl.multiple_of(i * sub, sub)
        top = (row_pos + row_start) == 0
        for start in range(0, columns_full, lane):

            def pick(component, odd_x, odd_y):
                def at(rows):
                    inner = kernel_ref[component, rows, start : start + lane]
                    if odd_y and start == 0:
                        edge = kernel_ref[component, rows, columns_full : columns_full + lane]
                        inner = jnp.where(lane_pos == 0, edge, inner)
                    return inner

                values = at(pl.ds(row_start, sub))
                if odd_x:
                    values = jnp.where(top, at(pl.ds(rows_full, sub)), values)
                return values

            spec = {}
            for px in range(2):
                for py in range(2):
                    for f in range(6):
                        spec[px, py, f] = spec_ref[
                            f,
                            pl.ds(row_start + px * rows_full, sub),
                            py * columns_full + start : py * columns_full + start + lane,
                        ]
            k_xy = pick(3, 0, 0)
            for px in range(2):
                for py in range(2):
                    sx = 1.0 if px else -1.0
                    sy = 1.0 if py else -1.0
                    k_xx, k_yy, k_zz = [pick(n, px, py) for n in range(3)]
                    k_xz = sx * pick(4, 0, py)
                    k_yz = sy * pick(5, px, 0)
                    xy_both = -(sx * sy) * k_xy
                    for part in range(2):
                        turn = 1.0 if part else -1.0
                        other = 1 - part
                        field_x = (
                            k_xx * spec[px, py, part]
                            + xy_both * spec[1 - px, 1 - py, 2 + part]
                            + turn * (k_xz * spec[1 - px, py, 4 + other])
                        )
                        field_y = (
                            xy_both * spec[1 - px, 1 - py, part]
                            + k_yy * spec[px, py, 2 + part]
                            + turn * (k_yz * spec[px, 1 - py, 4 + other])
                        )
                        field_z = k_zz * spec[px, py, 4 + part] + turn * (
                            k_xz * spec[1 - px, py, other] + k_yz * spec[px, 1 - py, 2 + other]
                        )
                        for c, field in enumerate((field_x, field_y, field_z)):
                            spec_ref[
                                2 * c + part,
                                pl.ds(row_start + px * rows_full, sub),
                                py * columns_full + start : py * columns_full + start + lane,
                            ] = field
        return carry

    lax.fori_loop(0, rows_full // sub, tensor, 0)

    def backward(f, carry):
        c, part = f // 2, f % 2
        upper, lower = split_limbs(spec_ref[f])
        lines = dot32(gx, jnp.concatenate([upper, lower, upper], axis=0))
        upper, lower = split_limbs(lines)
        cells = dot32(jnp.concatenate([upper, lower, upper], axis=1), gy)
        for g in range(groups):
            out_ref[g, c, part] = cells[g * slab : (g + 1) * slab]
        return carry

    lax.fori_loop(0, 6, backward, 0)


def swap_kernel(shifts, combine, tile_ref, out_ref, held_ref, send_sem, recv_sem):
    groups, images = lax.axis_size("space"), lax.axis_size("image")
    me, image = lax.axis_index("space"), lax.axis_index("image")
    routes = [
        (n, shift, d)
        for n, shift in enumerate(shifts)
        for d in range(groups)
        if shift != 0 or d != 0
    ]

    def target(shift, d):
        return {"image": lax.rem(image - shift + images, images), "space": lax.rem(me + d, groups)}

    barrier = pltpu.get_barrier_semaphore()
    for n, shift, d in routes:
        pl.semaphore_signal(
            barrier, inc=1, device_id=target(shift, d), device_id_type=pl.DeviceIdType.MESH
        )
    pl.semaphore_wait(barrier, len(routes))

    def copy_of(n, shift, d, slot):
        return pltpu.make_async_remote_copy(
            src_ref=tile_ref,
            dst_ref=held_ref.at[n, slot],
            send_sem=send_sem.at[n, d],
            recv_sem=recv_sem.at[n, d],
            device_id=target(shift, d),
            device_id_type=pl.DeviceIdType.MESH,
        )

    for n, shift, d in routes:
        copy_of(n, shift, d, me).start()
    held_ref[shifts.index(0), me] = tile_ref[...]
    for n, shift, d in routes:
        copy_of(n, shift, d, lax.rem(me + groups - d, groups)).wait_recv()
    for n in range(len(shifts)):
        total = held_ref[n, 0]
        for g in range(1, groups):
            total = combine(total, held_ref[n, g])
        out_ref[n] = total
    for n, shift, d in routes:
        copy_of(n, shift, d, me).wait_send()


def swapped(values, shifts, combine, collective_id):
    rows, columns = values.shape
    tile = jnp.pad(values, ((0, -rows % 8), (0, -columns % 128)))
    groups = lax.axis_size("space")
    inside = pl.BlockSpec(memory_space=pltpu.VMEM)
    result = pl.pallas_call(
        functools.partial(swap_kernel, shifts, combine),
        in_specs=[inside],
        out_specs=inside,
        out_shape=jax.ShapeDtypeStruct((len(shifts),) + tile.shape, jnp.float32),
        scratch_shapes=[
            pltpu.VMEM((len(shifts), groups) + tile.shape, jnp.float32),
            pltpu.SemaphoreType.DMA((len(shifts), groups)),
            pltpu.SemaphoreType.DMA((len(shifts), groups)),
        ],
        compiler_params=pltpu.CompilerParams(
            collective_id=collective_id, has_side_effects=True
        ),
        name="swap_kernel",
    )(tile)
    return result[:, :rows, :columns]


def demag_pair(magnet, kernel, images, early_work, pair_index):
    layer_count, row_count, column_count = magnet.shape[2:]
    groups = lax.axis_size("space")
    local_planes = 2 * layer_count // groups
    full_rows = row_count * groups
    plane_dims = (2 * layer_count, 3, 2, row_count, column_count)
    layer_spec = pl.BlockSpec((2, 1, layer_count, row_count, column_count), lambda c: (0, c, 0, 0, 0))
    plane_spec = pl.BlockSpec((2 * layer_count, 1, 2, row_count, column_count), lambda c: (0, c, 0, 0, 0))
    planes = pl.pallas_call(
        layers_to_planes,
        grid=(3,),
        in_specs=[layer_spec],
        out_specs=plane_spec,
        out_shape=jax.ShapeDtypeStruct(plane_dims, jnp.float32),
        name="layers_to_planes",
    )(magnet)
    planes = planes.reshape((groups, local_planes) + plane_dims[1:])
    table_y = parity_table(column_count)
    table_x = parity_table(full_rows)
    tables = [
        table_limbs(table_y),
        table_limbs(table_x.T),
        table_limbs(table_x * parity_weights(full_rows)[None, :]),
        table_limbs((table_y * parity_weights(column_count)[None, :]).T),
    ]
    slab_dims = (local_planes, groups, 3, 2, row_count, column_count)
    tensor_dims = (local_planes, 6, full_rows + 8, column_count + 128)
    anywhere = pl.BlockSpec(memory_space=pl.ANY)
    inside = pl.BlockSpec(memory_space=pltpu.VMEM)
    dots = 6 * local_planes * 4 * full_rows * column_count * 3 * (full_rows + column_count // 2)
    planes = pl.pallas_call(
        plane_kernel,
        in_specs=[anywhere, anywhere] + [inside] * len(tables),
        out_specs=anywhere,
        out_shape=jax.ShapeDtypeStruct(planes.shape, jnp.float32),
        scratch_shapes=[
            pltpu.VMEM((6, 2 * full_rows, 2 * column_count), jnp.float32),
            pltpu.VMEM(slab_dims, jnp.float32),
            pltpu.VMEM(tensor_dims, jnp.float32),
            pltpu.VMEM(slab_dims, jnp.float32),
            pltpu.SemaphoreType.DMA((local_planes, groups)),
            pltpu.SemaphoreType.DMA((local_planes, groups)),
            pltpu.SemaphoreType.DMA((local_planes,)),
            pltpu.SemaphoreType.DMA((local_planes,)),
            pltpu.SemaphoreType.DMA((local_planes,)),
        ],
        compiler_params=pltpu.CompilerParams(
            vmem_limit_bytes=56 * 1024 * 1024, collective_id=pair_index, has_side_effects=True
        ),
        cost_estimate=pl.CostEstimate(
            flops=4 * dots, bytes_accessed=4 * planes.size * 4, transcendentals=0
        ),
        name="plane_kernel",
    )(planes, kernel, *[jnp.asarray(t) for t in tables])
    planes = planes.reshape(plane_dims)
    planes, *images = lax.optimization_barrier((planes, *images))
    planes = lax.all_to_all(planes, "space", split_axis=0, concat_axis=0, tiled=True)
    planes, early = lax.optimization_barrier((planes, early_work(images)))
    padded_cells = 8 * layer_count * full_rows * column_count
    field = pl.pallas_call(
        functools.partial(planes_to_layers, -1.0 / padded_cells),
        grid=(3,),
        in_specs=[plane_spec],
        out_specs=layer_spec,
        out_shape=jax.ShapeDtypeStruct(magnet.shape, jnp.float32),
        name="planes_to_layers",
    )(planes)
    return field, images, early


def demag_field(magnet, kernel, images, early_work):
    fields = []
    for index, start in enumerate(range(0, magnet.shape[0], 2)):
        field, images, early = demag_pair(
            magnet[start : start + 2], kernel, images, early_work, index
        )
        fields.append(field)
    return (fields[0] if len(fields) == 1 else jnp.concatenate(fields, axis=0)), images, early


def local_fields(magnet, anisotropy, rimmed):
    layer_count = magnet.shape[2]
    row_count = magnet.shape[3]
    column_count = magnet.shape[4]
    x_plus = rimmed[:, :, :, 2:]
    x_minus = rimmed[:, :, :, :-2]
    padded = jnp.pad(magnet, ((0, 0), (0, 0), (1, 1), (0, 0), (1, 1)))
    z_plus = padded[:, :, 2:, :, 1:-1]
    z_minus = padded[:, :, :-2, :, 1:-1]
    y_plus = padded[:, :, 1:-1, :, 2:]
    y_minus = padded[:, :, 1:-1, :, :-2]
    first_row = lax.axis_index("space") * row_count
    full_rows = row_count * lax.axis_size("space")
    layer_pos = lax.broadcasted_iota(jnp.int32, (layer_count, row_count, column_count), 0)
    row_pos = lax.broadcasted_iota(jnp.int32, (layer_count, row_count, column_count), 1) + first_row
    column_pos = lax.broadcasted_iota(jnp.int32, (layer_count, row_count, column_count), 2)
    boundary = (layer_pos == 0).astype(jnp.float32) + (layer_pos == layer_count - 1).astype(
        jnp.float32
    )
    boundary = (
        boundary
        + (row_pos == 0).astype(jnp.float32)
        + (row_pos == full_rows - 1).astype(jnp.float32)
    )
    boundary = (
        boundary
        + (column_pos == 0).astype(jnp.float32)
        + (column_pos == column_count - 1).astype(jnp.float32)
    )
    present = 6.0 - boundary
    neighbours = x_plus + x_minus + y_plus + y_minus + z_plus + z_minus
    exchange_part = exchange_strength * (neighbours - present * magnet)
    chiral_x = chiral_strength * (x_plus[:, 2] - x_minus[:, 2])
    chiral_y = chiral_strength * (y_plus[:, 2] - y_minus[:, 2])
    chiral_z = -chiral_strength * (x_plus[:, 0] - x_minus[:, 0] + (y_plus[:, 1] - y_minus[:, 1]))
    easy_axis = 2.0 * anisotropy[:, None] * magnet[:, 2]
    local_part = exchange_part + jnp.stack([chiral_x, chiral_y, chiral_z + easy_axis], axis=1)
    return local_part


def body(magnet, anisotropy, kernel):
    image_count = magnet.shape[0]
    cell_count = magnet.shape[2] * magnet.shape[3] * lax.axis_size("space") * magnet.shape[4]
    framed = extended(magnet, (("image", 0),), 1)
    rimmed = extended(magnet, (("space", 3),), 1)

    def early_work(images):
        prior, following = images[0][:-2], images[0][2:]
        ahead = project(following - magnet, magnet)
        behind = project(magnet - prior, magnet)
        return (
            local_fields(magnet, anisotropy, images[1]),
            total_cells(angle_squared(magnet, following)),
            total_cells(ahead * ahead),
            total_cells(ahead * behind),
            total_cells(behind * behind),
        )

    demag, (framed, _), early = demag_field(magnet, kernel, [framed, rimmed], early_work)
    fields = early[0] + demag
    prior_image = framed[:-2]
    next_image = framed[2:]
    true_force = project(fields, magnet)
    tangent_next = project(next_image - magnet, magnet)
    tangent_prior = project(magnet - prior_image, magnet)
    sums = jnp.stack(
        [
            -0.5 * total_cells(magnet * fields),
            *early[1:],
            total_cells(true_force * tangent_next),
            total_cells(true_force * tangent_prior),
        ],
        axis=1,
    )
    band_size = image_count * lax.axis_size("image")
    swaps = swapped(sums, (-1, 0, 1), jnp.add, 64)
    band = jnp.concatenate([swaps[0, -1:], swaps[1], swaps[2, :1]], axis=0)
    energy_band, distance_band = band[:, 0], jnp.sqrt(band[:, 1] / cell_count)
    weight_next, weight_prior = tangent_weights(
        energy_band, jnp.roll(energy_band, -1), jnp.roll(energy_band, 1)
    )
    length_squares = (
        weight_next * weight_next * band[:, 2]
        + 2.0 * weight_next * weight_prior * band[:, 3]
        + weight_prior * weight_prior * band[:, 4]
    )
    drive_total = weight_next * band[:, 5] + weight_prior * band[:, 6]
    tangent_scale = jnp.sqrt(jnp.maximum(length_squares, 0.0) / cell_count + epsilon)
    parallel = drive_total / (cell_count * tangent_scale)
    spring = spring_strength * (distance_band - jnp.roll(distance_band, 1))
    first_image = lax.axis_index("image") * image_count
    image_index = first_image - 1 + jnp.arange(image_count + 2)
    interior = ((image_index > 0) & (image_index < band_size - 1)).astype(jnp.float32)
    pull = (spring - parallel) / tangent_scale
    mine = jnp.stack([energy_band, pull * weight_next, pull * weight_prior, interior], axis=1)[1:-1]
    energy_total = mine[:, 0]
    band_force = jnp.where(
        lift_axes(mine[:, 3]) > 0.0,
        true_force + lift_axes(mine[:, 1]) * tangent_next + lift_axes(mine[:, 2]) * tangent_prior,
        0.0,
    )
    local_largest = jnp.max(jnp.sqrt(jnp.sum(band_force * band_force, axis=1)), axis=(1, 2, 3))
    largest = swapped(local_largest[None, :], (0,), jnp.maximum, 65)[0, 0]
    move_scale = jnp.minimum(step_limit, rotation_limit / (largest + epsilon))
    stepped = magnet + lift_axes(move_scale) * band_force
    updated = stepped / jnp.sqrt(jnp.sum(stepped * stepped, axis=1, keepdims=True))
    return (updated, band_force, energy_total / cell_count)


def solution(mesh):
    in_specs = (P("image", None, None, "space", None), P("space"), P(None, "space", None, None))
    out_specs = (
        P("image", None, None, "space", None),
        P("image", None, None, "space", None),
        P("image"),
    )
    return jax.shard_map(body, mesh=mesh, in_specs=in_specs, out_specs=out_specs, check_vma=False)
```
